32 devices in a mesh: ty: 4 (over z), tx: 8 (over y, x, core).
Axes of the slice: x: 2, y: 2, z: 4, core: 2. Of those that a mesh axis runs over, the one named last changes fastest.
Arguments:
- x_tok: bfloat16 [8192, 1024], P('ty', 'tx')
- dy_tok: bfloat16 [8192, 1024], P('ty', 'tx')
- ln_gain: float32 [1024], P('tx')
- w_gate: bfloat16 [1024, 4096], P('tx', 'ty')
- w_up: bfloat16 [1024, 4096], P('tx', 'ty')
- w_down: bfloat16 [4096, 1024], P('ty', 'tx')
Outputs:
- output 1: bfloat16 [8192, 1024], P('ty', 'tx')
- output 2: bfloat16 [8192, 1024], P('ty', 'tx')
- output 3: float32 [1024, 4096], P('tx', 'ty')
- output 4: float32 [1024, 4096], P('tx', 'ty')
- output 5: float32 [4096, 1024], P('ty', 'tx')
- output 6: float32 [1024], P('tx')
All inputs are finite; a program needn't handle non-finite values.
Results may differ from the reference program's by a relative error of at most 0.001.
Values are sent between devices in bfloat16 or wider.
A program may use at most 1 GiB of HBM per device.

```python
import jax
import jax.numpy as jnp
from jax import lax

TOKENS = 8192
D_MODEL = 1024
D_FF = 4096
LN_EPS = 1e-6


def setup_inputs(seed: int = 0) -> dict:
    key_list = jax.random.split(jax.random.key(seed), 9)
    x_tok = (jax.random.normal(key_list[0], (TOKENS, D_MODEL), jnp.float32)
             + 1.5 * jax.random.normal(key_list[1], (TOKENS, 1), jnp.float32)).astype(jnp.bfloat16)
    dy_tok = jax.random.normal(key_list[2], (TOKENS, D_MODEL), jnp.float32).astype(jnp.bfloat16)
    ln_gain = 1.0 + 0.5 * jax.random.normal(key_list[3], (D_MODEL,), jnp.float32)
    in_scale = D_MODEL ** -0.5
    w_gate = ((jax.random.normal(key_list[4], (D_MODEL, D_FF), jnp.float32)
               + jax.random.normal(key_list[5], (1, D_FF), jnp.float32)) * in_scale).astype(jnp.bfloat16)
    w_up = ((jax.random.normal(key_list[6], (D_MODEL, D_FF), jnp.float32)
             + jax.random.normal(key_list[7], (1, D_FF), jnp.float32)) * in_scale).astype(jnp.bfloat16)
    w_down = (jax.random.normal(key_list[8], (D_FF, D_MODEL), jnp.float32) * D_FF ** -0.5).astype(jnp.bfloat16)
    return {"x_tok": x_tok, "dy_tok": dy_tok, "ln_gain": ln_gain,
            "w_gate": w_gate, "w_up": w_up, "w_down": w_down}


def reference(x_tok, dy_tok, ln_gain, w_gate, w_up, w_down):
    x_float = x_tok.astype(jnp.float32)
    mean_x = jnp.mean(x_float, axis=1, keepdims=True)
    mean_sq = jnp.mean(x_float * x_float, axis=1, keepdims=True)
    inv_std = lax.rsqrt(mean_sq - mean_x * mean_x + LN_EPS)
    x_hat = (x_float - mean_x) * inv_std
    h_norm = (ln_gain * x_hat).astype(jnp.bfloat16)
    gate_pre = jnp.dot(h_norm, w_gate, preferred_element_type=jnp.float32)
    up_pre = jnp.dot(h_norm, w_up, preferred_element_type=jnp.float32)
    gate_sig = jax.nn.sigmoid(gate_pre)
    gate_swish = gate_pre * gate_sig
    act_out = (gate_swish * up_pre).astype(jnp.bfloat16)
    mlp_out = jnp.dot(act_out, w_down, preferred_element_type=jnp.float32)
    y_tok = (x_float + mlp_out).astype(jnp.bfloat16)
    dw_down = jnp.dot(act_out.T, dy_tok, preferred_element_type=jnp.float32)
    d_act = jnp.dot(dy_tok, w_down.T, preferred_element_type=jnp.float32)
    d_gate = (d_act * up_pre * gate_sig * (1.0 + gate_pre * (1.0 - gate_sig))).astype(jnp.bfloat16)
    d_up = (d_act * gate_swish).astype(jnp.bfloat16)
    dw_gate = jnp.dot(h_norm.T, d_gate, preferred_element_type=jnp.float32)
    dw_up = jnp.dot(h_norm.T, d_up, preferred_element_type=jnp.float32)
    d_hnorm = (jnp.dot(d_gate, w_gate.T, preferred_element_type=jnp.float32)
               + jnp.dot(d_up, w_up.T, preferred_element_type=jnp.float32))
    d_gain = jnp.sum(d_hnorm * x_hat, axis=0)
    d_xhat = d_hnorm * ln_gain
    dx_ln = inv_std * (d_xhat - jnp.mean(d_xhat, axis=1, keepdims=True)
                       - x_hat * jnp.mean(d_xhat * x_hat, axis=1, keepdims=True))
    dx_tok = (dy_tok.astype(jnp.float32) + dx_ln).astype(jnp.bfloat16)
    return (y_tok, dx_tok, dw_gate, dw_up, dw_down, d_gain)
```

```python
import functools

import jax
import jax.numpy as jnp
from jax import lax
from jax.experimental import pallas as pl
from jax.experimental.pallas import tpu as pltpu
from jax.sharding import PartitionSpec as P

LN_EPS = 1e-6
F32 = jnp.float32
BF16 = jnp.bfloat16
MESH = pl.DeviceIdType.MESH
LANE = 128


def place():
    z = lax.axis_index("ty")
    t = lax.axis_index("tx")
    core = lax.rem(t, 2)
    xbit = lax.rem(lax.div(t, 2), 2)
    ybit = lax.div(t, 4)
    flips = (1 - 2 * core, 2 - 4 * xbit, 4 - 8 * ybit)

    def peer(s):
        out = t
        for bit in range(3):
            if s >> bit & 1:
                out = out + flips[bit]
        return out

    return z, t, peer


def cols(k, width=LANE):
    return pl.ds(pl.multiple_of(k * width, width), width)


class Sends:
    def __init__(self, send_sem, recv_sem):
        self.send_sem, self.recv_sem, self.count, self.started = send_sem, recv_sem, 0, []

    def slot(self):
        self.count += 1
        return self.count - 1

    def copy(self, src, dst, slot, device):
        return pltpu.make_async_remote_copy(src_ref=src, dst_ref=dst, send_sem=self.send_sem.at[slot],
                                            recv_sem=self.recv_sem.at[slot], device_id=device, device_id_type=MESH)


def gather_kernel(x_in, dy_in, g_in, w1_in, w3_in, w2_in,
                  h_out, dy_all, x_rows, gain_all, w1_all, w3_all, w2_all,
                  x_all, send_sem, recv_sem, local_sem):
    z, t, peer = place()
    tokens = x_all.shape[0]
    half = tokens // 2
    net = Sends(send_sem, recv_sem)
    pending = []

    def send(src, dst, slot, device):
        c = net.copy(src, dst, slot, device)
        c.start()
        pending.append(c)

    def arrived(dst, slot):
        net.copy(dst, dst, slot, (z, peer(1))).wait_recv()

    locals_ = [
        pltpu.make_async_copy(x_in, x_all.at[:, cols(t)], local_sem.at[0]),
        pltpu.make_async_copy(dy_in, dy_all.at[:, cols(t)], local_sem.at[1]),
        pltpu.make_async_copy(g_in, gain_all.at[:, cols(t)], local_sem.at[2]),
        pltpu.make_async_copy(w1_in.at[:, cols(t)], w1_all.at[cols(t), cols(z)], local_sem.at[3]),
        pltpu.make_async_copy(w3_in.at[:, cols(t)], w3_all.at[cols(t), cols(z)], local_sem.at[4]),
        pltpu.make_async_copy(w2_in.at[cols(t), :], w2_all.at[cols(z), cols(t)], local_sem.at[5]),
    ]
    for c in locals_:
        c.start()

    w_slots = {}
    for s in (6, 7, 2, 3, 4, 5, 1):
        p = peer(s)
        w_slots[s] = [net.slot() for _ in range(4)]
        a, b, c, d = w_slots[s]
        send(w1_in.at[:, cols(p)], w1_all.at[cols(t), cols(z)], a, (z, p))
        send(w3_in.at[:, cols(p)], w3_all.at[cols(t), cols(z)], b, (z, p))
        send(w2_in.at[cols(p), :], w2_all.at[cols(z), cols(t)], c, (z, p))
        send(g_in, gain_all.at[:, cols(t)], d, (z, p))

    lo, hi = pl.ds(0, half), pl.ds(half, half)
    px, py, pd, pc = peer(2), peer(4), peer(6), peer(1)

    def plane_first(src, full, sl):
        send(src.at[lo], full.at[lo, cols(t)], sl[0], (z, px))
        send(src.at[hi], full.at[hi, cols(t)], sl[2], (z, py))
        send(src.at[hi], full.at[hi, cols(t)], sl[1], (z, px))
        send(src.at[lo], full.at[lo, cols(t)], sl[3], (z, py))
        send(src, full.at[:, cols(t)], sl[4], (z, pc))

    def plane_forward(full, sl):
        arrived(full.at[lo, cols(px)], sl[0])
        send(full.at[lo, cols(px)], full.at[lo, cols(px)], sl[5], (z, py))
        send(full.at[lo, cols(px)], full.at[lo, cols(px)], sl[7], (z, pc))
        arrived(full.at[hi, cols(py)], sl[2])
        send(full.at[hi, cols(py)], full.at[hi, cols(py)], sl[6], (z, px))
        send(full.at[hi, cols(py)], full.at[hi, cols(py)], sl[9], (z, pc))

    def plane_rest(full, sl):
        arrived(full.at[hi, cols(px)], sl[1])
        send(full.at[hi, cols(px)], full.at[hi, cols(px)], sl[8], (z, pc))
        arrived(full.at[lo, cols(py)], sl[3])
        send(full.at[lo, cols(py)], full.at[lo, cols(py)], sl[10], (z, pc))
        arrived(full.at[lo, cols(pd)], sl[5])
        send(full.at[lo, cols(pd)], full.at[lo, cols(pd)], sl[11], (z, pc))
        arrived(full.at[hi, cols(pd)], sl[6])
        send(full.at[hi, cols(pd)], full.at[hi, cols(pd)], sl[12], (z, pc))

    def plane_last(full, sl):
        arrived(full.at[:, cols(pc)], sl[4])
        arrived(full.at[lo, cols(peer(3))], sl[7])
        arrived(full.at[hi, cols(peer(3))], sl[8])
        arrived(full.at[hi, cols(peer(5))], sl[9])
        arrived(full.at[lo, cols(peer(5))], sl[10])
        arrived(full.at[lo, cols(peer(7))], sl[11])
        arrived(full.at[hi, cols(peer(7))], sl[12])

    sx = [net.slot() for _ in range(13)]
    sd = [net.slot() for _ in range(13)]
    plane_first(x_in, x_all, sx)

    for c in locals_[2:]:
        c.wait()
    for s in (6, 7, 2, 3, 4, 5, 1):
        p = peer(s)
        a, b, c, d = w_slots[s]
        arrived(w1_all.at[cols(p), cols(z)], a)
        arrived(w3_all.at[cols(p), cols(z)], b)
        arrived(w2_all.at[cols(z), cols(p)], c)
        arrived(gain_all.at[:, cols(p)], d)

    n_z = 4
    up = [[net.slot() for _ in range(3)] for _ in range(n_z)]
    down = [[net.slot() for _ in range(3)] for _ in range(n_z)]

    def chunk(k):
        return (w1_all.at[:, pl.ds(k * LANE, LANE)], w3_all.at[:, pl.ds(k * LANE, LANE)],
                w2_all.at[pl.ds(k * LANE, LANE), :])

    def pass_on(here, k, upward):
        slots = (up if upward else down)[k]
        nxt = here + 1 if upward else here - 1

        @pl.when(z == here)
        def _():
            for ref, slot in zip(chunk(k), slots):
                net.copy(ref, ref, slot, (nxt, t)).start()

    def take(here, k):
        @pl.when(z == here)
        def _():
            for ref, slot in zip(chunk(k), (up if k < here else down)[k]):
                net.copy(ref, ref, slot, (here, pc)).wait_recv()

    for here in range(n_z):
        if here + 1 < n_z:
            pass_on(here, here, True)
        if here > 0:
            pass_on(here, here, False)

    plane_forward(x_all, sx)
    plane_first(dy_in, dy_all, sd)
    plane_rest(x_all, sx)
    locals_[0].wait()
    plane_last(x_all, sx)

    def norm_tile(i, _):
        rows = pl.ds(i * 256, 256)
        xf = x_all[rows, :].astype(F32)
        d = xf.shape[1]
        mu = jnp.sum(xf, axis=1, keepdims=True) / d
        sq = jnp.sum(xf * xf, axis=1, keepdims=True) / d
        r = lax.rsqrt(sq - mu * mu + LN_EPS)
        h_out[rows, :] = (gain_all[0:1, :] * ((xf - mu) * r)).astype(BF16)
        return 0

    for here in range(n_z):
        for k in (here - 1, here + 1):
            if 0 <= k < n_z:
                take(here, k)
                nxt = 2 * here - k
                if 0 <= nxt < n_z:
                    pass_on(here, k, nxt > here)

    lax.fori_loop(0, tokens // 256, norm_tile, 0)
    own_rows = tokens // 8
    x_rows[...] = x_all[pl.ds(pl.multiple_of(t * own_rows, own_rows), own_rows), :]
    plane_forward(dy_all, sd)
    plane_rest(dy_all, sd)
    for dist in (2, 3):
        for here in range(n_z):
            for k in (here - dist, here + dist):
                if 0 <= k < n_z:
                    take(here, k)
                    nxt = here + (1 if k < here else -1)
                    if 0 <= nxt < n_z:
                        pass_on(here, k, nxt > here)
    locals_[1].wait()
    plane_last(dy_all, sd)
    for c in pending:
        c.wait_send()
    for here in range(n_z):
        for upward in (True, False):
            nxt = here + 1 if upward else here - 1
            if 0 <= nxt < n_z:
                for k in (range(here + 1) if upward else range(here, n_z)):
                    @pl.when(z == here)
                    def _(k=k, upward=upward, nxt=nxt):
                        for ref, slot in zip(chunk(k), (up if upward else down)[k]):
                            net.copy(ref, ref, slot, (nxt, t)).wait_send()


N_GATHER = 28 + 26 + 24


def reduce_kernel(m_in, dh_in, w1_in, w3_in, w2_in, x_rows, dy_rows, gain_all,
                  y_out, dx_out, dw1_out, dw3_out, dw2_out, dg_out,
                  m0, m1, m2, e0, e1, e2, out1, out3, out2, in1, in3, in2,
                  y_rows, dx_rows, dg_rows, dg_plane, dg_line,
                  send_sem, recv_sem, local_sem):
    z, t, peer = place()
    net = Sends(send_sem, recv_sem)
    rows = m0.shape[1]
    hr = rows // 2
    px, py, pd, pc = peer(2), peer(4), peer(6), peer(1)
    pending = []
    local_pending = []

    def send(src, dst, slot, device):
        c = net.copy(src, dst, slot, device)
        c.start()
        pending.append(c)

    def arrived(dst, slot):
        net.copy(dst, dst, slot, (z, pc)).wait_recv()

    def block(p):
        return pl.ds(pl.multiple_of(p * rows, rows), rows)

    is_end = jnp.logical_or(z == 0, z == 3)
    is_mid = jnp.logical_or(z == 1, z == 2)
    low = lax.div(3 - z, 2)
    c_end = 3 - 3 * low
    c_mid = 2 - low
    c_mid2 = 3 - c_mid
    c_end2 = 3 - c_end
    inner = z + 2 * low - 1
    outer = z - 2 * low + 1

    mine = ((w1_in, 0), (w3_in, 0), (w2_in, 1))

    def own(p, k):
        ref, axis = mine[p]
        return ref.at[:, cols(k)] if axis == 0 else ref.at[cols(k), :]

    outs = (out1, out3, out2)
    ins = (in1, in3, in2)
    out_slots = [[net.slot() for _ in range(3)] for _ in range(3)]
    in_slots = [[net.slot() for _ in range(3)] for _ in range(2)]
    end_slots = [net.slot() for _ in range(3)]

    @pl.when(is_end)
    def _():
        for q, k in enumerate((c_mid2, c_end2, c_mid)):
            for p in range(3):
                net.copy(own(p, k), outs[p].at[q], out_slots[q][p], (inner, t)).start()

    fin_slots = {s: [net.slot() for _ in range(3)] for s in range(1, 8)}

    def finish_piece(p, src):
        for s in (6, 7, 2, 3, 4, 5, 1):
            q = peer(s)
            if p < 2:
                c = net.copy(src.at[cols(q), :], (dw1_out, dw3_out)[p].at[:, cols(t)], fin_slots[s][p], (z, q))
            else:
                c = net.copy(src.at[:, cols(q)], dw2_out.at[cols(t), :], fin_slots[s][p], (z, q))
            c.start()
        if p < 2:
            pltpu.make_async_copy(src.at[cols(t), :], (dw1_out, dw3_out)[p].at[:, cols(t)], local_sem.at[p]).start()
        else:
            pltpu.make_async_copy(src.at[:, cols(t)], dw2_out.at[cols(t), :], local_sem.at[p]).start()

    def from_outer(q, p, k):
        @pl.when(is_mid)
        def _():
            dst = outs[p].at[q]
            arrived(dst, out_slots[q][p])
            dst[...] += own(p, k)[...]
            net.copy(dst, ins[p].at[q], in_slots[q][p], (inner, t)).start()

    def to_end(p):
        @pl.when(is_mid)
        def _():
            dst = ins[p].at[1]
            arrived(dst, in_slots[1][p])
            dst[...] += own(p, c_end)[...]
            net.copy(dst, dst, end_slots[p], (outer, t)).start()

    def last_mid(p):
        @pl.when(is_mid)
        def _():
            a, b = outs[p].at[2], ins[p].at[0]
            arrived(b, in_slots[0][p])
            arrived(a, out_slots[2][p])
            a[...] += b[...] + own(p, c_mid)[...]
            finish_piece(p, a)

    def last_end(p):
        @pl.when(is_end)
        def _():
            a = ins[p].at[1]
            arrived(a, end_slots[p])
            a[...] += own(p, c_end)[...]
            finish_piece(p, a)

    keep = (t, px, py, pd)
    away = (pc, peer(3), peer(5), peer(7))

    def stage0_start(src, r0, sl):
        for j in (3, 1, 2, 0):
            send(src.at[block(away[j]), :], r0.at[j], sl[j], (z, pc))

    def stage1(src, r0, r1, sl):
        for j in (3, 1, 2, 0):
            arrived(r0.at[j], sl[j])
            r0[j] += src[block(keep[j]), :]
            if j == 3:
                send(r0.at[3, pl.ds(0, hr)], r1.at[0], sl[4], (z, px))
                send(r0.at[3, pl.ds(hr, hr)], r1.at[1], sl[5], (z, py))
            if j == 1:
                send(r0.at[1, pl.ds(0, hr)], r1.at[2], sl[6], (z, px))
            if j == 2:
                send(r0.at[2, pl.ds(hr, hr)], r1.at[3], sl[7], (z, py))

    def stage2(r0, r1, r2, sl):
        arrived(r1.at[0], sl[4])
        r0[2, 0:hr] += r1[0]
        send(r0.at[2, pl.ds(0, hr)], r2.at[0], sl[8], (z, py))
        arrived(r1.at[1], sl[5])
        r0[1, hr:rows] += r1[1]
        send(r0.at[1, pl.ds(hr, hr)], r2.at[1], sl[9], (z, px))

    def stage3(r0, r1, sl):
        arrived(r1.at[2], sl[6])
        r0[0, 0:hr] += r1[2]
        arrived(r1.at[3], sl[7])
        r0[0, hr:rows] += r1[3]

    def stage4(r0, r2, sl):
        arrived(r2.at[0], sl[8])
        r0[0, 0:hr] += r2[0]
        arrived(r2.at[1], sl[9])
        r0[0, hr:rows] += r2[1]

    sm = [net.slot() for _ in range(10)]
    se = [net.slot() for _ in range(10)]
    sy = {s: net.slot() for s in range(1, 8)}
    sdx = {s: net.slot() for s in range(1, 8)}
    sg = {s: net.slot() for s in range(1, 8)}
    sz = {s: net.slot() for s in range(1, 4)}

    def spread(src, dst, slots, local):
        for s in (6, 7, 2, 3, 4, 5, 1):
            q = peer(s)
            send(src.at[:, cols(q)], dst.at[block(t), :], slots[s], (z, q))
        c = pltpu.make_async_copy(src.at[:, cols(t)], dst.at[block(t), :], local_sem.at[local])
        c.start()
        local_pending.append(c)

    stage0_start(m_in, m0, sm)
    stage0_start(dh_in, e0, se)
    stage1(m_in, m0, m1, sm)
    from_outer(0, 0, c_mid2)
    stage2(m0, m1, m2, sm)
    stage1(dh_in, e0, e1, se)
    from_outer(0, 1, c_mid2)
    stage3(m0, m1, sm)
    from_outer(0, 2, c_mid2)
    stage4(m0, m2, sm)
    y_rows[...] = (x_rows[...].astype(F32) + m0[0]).astype(BF16)
    spread(y_rows, y_out, sy, 3)
    from_outer(1, 0, c_end2)
    stage2(e0, e1, e2, se)
    from_outer(1, 1, c_end2)
    to_end(0)
    stage3(e0, e1, se)
    from_outer(1, 2, c_end2)
    to_end(1)
    stage4(e0, e2, se)

    xf = x_rows[...].astype(F32)
    d = xf.shape[1]
    mu = jnp.sum(xf, axis=1, keepdims=True) / d
    sq = jnp.sum(xf * xf, axis=1, keepdims=True) / d
    r = lax.rsqrt(sq - mu * mu + LN_EPS)
    xhat = (xf - mu) * r
    dh = e0[0]
    e = dh * gain_all[0:1, :]
    e_mean = jnp.sum(e, axis=1, keepdims=True) / d
    ex_mean = jnp.sum(e * xhat, axis=1, keepdims=True) / d
    dx_rows[...] = (dy_rows[...].astype(F32) + r * (e - e_mean - xhat * ex_mean)).astype(BF16)
    dg_rows[...] = jnp.sum((dh * xhat).reshape(rows // 8, 8, d), axis=0)
    spread(dx_rows, dx_out, sdx, 4)
    for s in range(1, 8):
        q = peer(s)
        send(dg_rows.at[:, cols(q)], dg_plane.at[s - 1], sg[s], (z, q))
    to_end(2)
    last_end(0)
    total = dg_rows[:, cols(t)]
    for s in range(1, 8):
        arrived(dg_plane.at[s - 1], sg[s])
        total = total + dg_plane[s - 1]
    dg_line[0] = total
    for s in range(1, 4):
        send(dg_line.at[0], dg_line.at[s], sz[s], (lax.rem(z + s, 4), t))
    last_end(1)
    last_end(2)
    last_mid(0)
    for s in range(1, 4):
        arrived(dg_line.at[s], sz[s])
    ordered = [dg_line[lax.rem(z - s + 4, 4)] for s in range(4)]
    dg_out[...] = (ordered[0] + ordered[1]) + (ordered[2] + ordered[3])
    last_mid(1)
    last_mid(2)

    for s in range(1, 8):
        q = peer(s)
        arrived(y_out.at[block(q), :], sy[s])
        arrived(dx_out.at[block(q), :], sdx[s])
        arrived(dw1_out.at[:, cols(q)], fin_slots[s][0])
        arrived(dw3_out.at[:, cols(q)], fin_slots[s][1])
        arrived(dw2_out.at[cols(q), :], fin_slots[s][2])
    for c in pending:
        c.wait_send()
    for c in local_pending:
        c.wait()
    for p in range(3):
        if p < 2:
            pltpu.make_async_copy(outs[p].at[2, cols(t), :], (dw1_out, dw3_out)[p].at[:, cols(t)], local_sem.at[p]).wait()
        else:
            pltpu.make_async_copy(outs[p].at[2, :, cols(t)], dw2_out.at[cols(t), :], local_sem.at[p]).wait()
        for s in range(1, 8):
            if p < 2:
                net.copy(outs[p].at[2, cols(t), :], (dw1_out, dw3_out)[p].at[:, cols(t)], fin_slots[s][p], (z, pc)).wait_send()
            else:
                net.copy(outs[p].at[2, :, cols(t)], dw2_out.at[cols(t), :], fin_slots[s][p], (z, pc)).wait_send()

    @pl.when(is_end)
    def _():
        for q, k in enumerate((c_mid2, c_end2, c_mid)):
            for p in range(3):
                net.copy(own(p, k), outs[p].at[q], out_slots[q][p], (inner, t)).wait_send()

    @pl.when(is_mid)
    def _():
        for p in range(3):
            for q in range(2):
                net.copy(outs[p].at[q], ins[p].at[q], in_slots[q][p], (inner, t)).wait_send()
            net.copy(ins[p].at[1], ins[p].at[1], end_slots[p], (outer, t)).wait_send()


N_REDUCE = 9 + 9 + 21 + 20 + 21 + 3


def contract_rows(a, b):
    return lax.dot_general(a, b, (((0,), (0,)), ((), ())), preferred_element_type=F32)


def contract_cols(a, b):
    return lax.dot_general(a, b, (((1,), (1,)), ((), ())), preferred_element_type=F32)


def solution(mesh):
    n_t = mesh.shape["tx"]
    n_z = mesh.shape["ty"]

    def local_step(x_blk, dy_blk, gain_blk, w1_blk, w3_blk, w2_blk):
        tokens, lane = x_blk.shape
        d = lane * n_t
        f = w1_blk.shape[1] // n_t * n_z
        rows = tokens // n_t
        gain8 = jnp.broadcast_to(gain_blk[None, :], (8, lane))
        any_spec = pl.BlockSpec(memory_space=pl.ANY)
        vmem = pl.BlockSpec(memory_space=pltpu.VMEM)
        s = jax.ShapeDtypeStruct
        h, dy_all, x_rows, gain_all, w1, w3, w2 = pl.pallas_call(
            gather_kernel,
            out_shape=(s((tokens, d), BF16), s((tokens, d), BF16), s((rows, d), BF16), s((8, d), F32),
                       s((d, f), BF16), s((d, f), BF16), s((f, d), BF16)),
            in_specs=[any_spec] * 6,
            out_specs=[vmem] * 7,
            scratch_shapes=[pltpu.VMEM((tokens, d), BF16), pltpu.SemaphoreType.DMA((N_GATHER,)),
                            pltpu.SemaphoreType.DMA((N_GATHER,)), pltpu.SemaphoreType.DMA((6,))],
            compiler_params=pltpu.CompilerParams(has_side_effects=True, vmem_limit_bytes=48 * 2**20),
            name="gather",
        )(x_blk, dy_blk, gain8, w1_blk, w3_blk, w2_blk)

        u = jnp.dot(h, w1, preferred_element_type=F32)
        v = jnp.dot(h, w3, preferred_element_type=F32)
        sig = jax.nn.sigmoid(u)
        swish = u * sig
        act = (swish * v).astype(BF16)
        da = contract_cols(dy_all, w2)
        du = (da * v * sig * (1.0 + u * (1.0 - sig))).astype(BF16)
        dv = (da * swish).astype(BF16)
        dw2 = contract_rows(act, dy_all)
        dw1 = contract_rows(h, du)
        dw3 = contract_rows(h, dv)
        m = jnp.dot(act, w2, preferred_element_type=F32)
        dh = contract_cols(du, w1) + contract_cols(dv, w3)
        dy_rows = lax.dynamic_slice(dy_all, (lax.axis_index("tx") * rows, 0), (rows, d))

        y, dx, dw1_o, dw3_o, dw2_o, dg = pl.pallas_call(
            reduce_kernel,
            out_shape=(s((tokens, lane), BF16), s((tokens, lane), BF16), s((lane, w1_blk.shape[1]), F32),
                       s((lane, w1_blk.shape[1]), F32), s((w1_blk.shape[1], lane), F32), s((8, lane), F32)),
            in_specs=[vmem] * 8,
            out_specs=[any_spec] * 5 + [vmem],
            scratch_shapes=[
                pltpu.VMEM((4, rows, d), F32), pltpu.VMEM((4, rows // 2, d), F32), pltpu.VMEM((2, rows // 2, d), F32),
                pltpu.VMEM((4, rows, d), F32), pltpu.VMEM((4, rows // 2, d), F32), pltpu.VMEM((2, rows // 2, d), F32),
                pltpu.VMEM((3, d, lane), F32), pltpu.VMEM((3, d, lane), F32), pltpu.VMEM((3, lane, d), F32),
                pltpu.VMEM((2, d, lane), F32), pltpu.VMEM((2, d, lane), F32), pltpu.VMEM((2, lane, d), F32),
                pltpu.VMEM((rows, d), BF16), pltpu.VMEM((rows, d), BF16), pltpu.VMEM((8, d), F32),
                pltpu.VMEM((7, 8, lane), F32), pltpu.VMEM((4, 8, lane), F32),
                pltpu.SemaphoreType.DMA((N_REDUCE,)), pltpu.SemaphoreType.DMA((N_REDUCE,)),
                pltpu.SemaphoreType.DMA((5,))],
            compiler_params=pltpu.CompilerParams(has_side_effects=True, vmem_limit_bytes=62 * 2**20),
            name="reduce",
        )(m, dh, dw1, dw3, dw2, x_rows, dy_rows, gain_all)
        return y, dx, dw1_o, dw3_o, dw2_o, jnp.sum(dg, axis=0)

    return jax.shard_map(
        local_step, mesh=mesh,
        in_specs=(P("ty", "tx"), P("ty", "tx"), P("tx"), P("tx", "ty"), P("tx", "ty"), P("ty", "tx")),
        out_specs=(P("ty", "tx"), P("ty", "tx"), P("tx", "ty"), P("tx", "ty"), P("ty", "tx"), P("tx")),
        check_vma=False)
```

```python
import jax
import jax.numpy as jnp
from jax import lax
from jax.experimental import pallas as pl
from jax.experimental.pallas import tpu as pltpu
from jax.sharding import PartitionSpec as P

LN_EPS = 1e-6
F32 = jnp.float32
BF16 = jnp.bfloat16
MESH = pl.DeviceIdType.MESH
LANE = 128
N_T = 8
N_Z = 4
PIECES = 6
ROWS = 384 // PIECES


def cols(k, width=LANE):
    return pl.ds(pl.multiple_of(k * width, width), width)


def dot(a, b):
    return jnp.dot(a, b, preferred_element_type=F32)


def dot_cols(a, b):
    return lax.dot_general(a, b, (((1,), (1,)), ((), ())), preferred_element_type=F32)


N_PLANE = 28 + 26
N_RED = 20 + 21 + 3
N_SUM = 6 * PIECES


def step_kernel(x_in, dy_in, g_in, w1_in, w3_in, w2_in,
                y_out, dx_out, dw_out, dg_out,
                x_all, h_all, dy_all, gain_all, w13, w2, act, act_t, duv_t, dw,
                m_away, m0, m1, m2, e_away, e0, e1, e2, outs, ins,
                x_rows, y_rows, dx_rows, dg_rows, dg_plane, dg_line,
                send_sem, recv_sem, wz_send, wz_recv, sum_send, sum_recv, fin_send, fin_recv,
                red_send, red_recv, local_sem):
    z = lax.axis_index("ty")
    t = lax.axis_index("tx")
    core = lax.rem(t, 2)
    xbit = lax.rem(lax.div(t, 2), 2)
    ybit = lax.div(t, 4)
    flips = (1 - 2 * core, 2 - 4 * xbit, 4 - 8 * ybit)
    duv = x_all

    def peer(s):
        out = t
        for bit in range(3):
            if s >> bit & 1:
                out = out + flips[bit]
        return out

    px, py, pd, pc = peer(2), peer(4), peer(6), peer(1)
    order = (2, 4, 3, 5, 6, 7, 1)
    tokens = x_all.shape[0]
    half = tokens // 2
    rows = tokens // N_T
    hr = rows // 2

    low = lax.div(3 - z, 2)
    is_end = jnp.logical_or(z == 0, z == 3)
    is_mid = jnp.logical_or(z == 1, z == 2)
    c_end = 3 - 3 * low
    c_mid = 2 - low
    c_mid2 = 3 - c_mid
    c_end2 = 3 - c_end
    inner = z + 2 * low - 1
    outer = z - 2 * low + 1

    def rcopy(src, dst, ssem, rsem, device):
        return pltpu.make_async_remote_copy(src_ref=src, dst_ref=dst, send_sem=ssem, recv_sem=rsem,
                                            device_id=device, device_id_type=MESH)

    count = [0]

    def slot():
        count[0] += 1
        return count[0] - 1

    pending = []

    def send(src, dst, sl, device):
        c = rcopy(src, dst, send_sem.at[sl], recv_sem.at[sl], device)
        c.start()
        pending.append(c)
        return c

    def arrived(dst, sl):
        rcopy(dst, dst, send_sem.at[sl], recv_sem.at[sl], (z, pc)).wait_recv()

    loc = [
        pltpu.make_async_copy(w1_in.at[:, cols(t)], w13.at[cols(t), cols(2 * z)], local_sem.at[0]),
        pltpu.make_async_copy(w3_in.at[:, cols(t)], w13.at[cols(t), cols(2 * z + 1)], local_sem.at[1]),
        pltpu.make_async_copy(w2_in.at[cols(t), :], w2.at[cols(z), cols(t)], local_sem.at[2]),
        pltpu.make_async_copy(g_in, gain_all.at[:, cols(t)], local_sem.at[3]),
        pltpu.make_async_copy(x_in, x_all.at[:, cols(t)], local_sem.at[4]),
        pltpu.make_async_copy(dy_in, dy_all.at[:, cols(t)], local_sem.at[5]),
    ]
    for c in loc:
        c.start()

    w_slots = {}
    for s in order:
        p = peer(s)
        w_slots[s] = [slot() for _ in range(4)]
        a, b, c, d = w_slots[s]
        send(w1_in.at[:, cols(p)], w13.at[cols(t), cols(2 * z)], a, (z, p))
        send(w3_in.at[:, cols(p)], w13.at[cols(t), cols(2 * z + 1)], b, (z, p))
        send(w2_in.at[cols(p), :], w2.at[cols(z), cols(t)], c, (z, p))
        send(g_in, gain_all.at[:, cols(t)], d, (z, p))

    lo, hi = pl.ds(0, half), pl.ds(half, half)

    def plane_first(src, full, sl):
        return [send(src.at[lo], full.at[lo, cols(t)], sl[0], (z, px)),
                send(src.at[hi], full.at[hi, cols(t)], sl[2], (z, py)),
                send(src.at[hi], full.at[hi, cols(t)], sl[1], (z, px)),
                send(src.at[lo], full.at[lo, cols(t)], sl[3], (z, py)),
                send(src, full.at[:, cols(t)], sl[4], (z, pc))]

    def forward(ref, sl, device):
        return send(ref, ref, sl, (z, device))

    def plane_forward(full, sl):
        a, b = full.at[lo, cols(px)], full.at[hi, cols(py)]
        arrived(a, sl[0])
        out = [forward(a, sl[5], py), forward(a, sl[7], pc)]
        arrived(b, sl[2])
        return out + [forward(b, sl[6], px), forward(b, sl[9], pc)]

    def plane_rest(full, sl):
        out = []
        for rr, p, i, o in ((hi, px, 1, 8), (lo, py, 3, 10), (lo, pd, 5, 11), (hi, pd, 6, 12)):
            ref = full.at[rr, cols(p)]
            arrived(ref, sl[i])
            out.append(forward(ref, sl[o], pc))
        return out

    def plane_last(full, sl):
        arrived(full.at[:, cols(pc)], sl[4])
        for rr, s, i in ((lo, 3, 7), (hi, 3, 8), (hi, 5, 9), (lo, 5, 10), (lo, 7, 11), (hi, 7, 12)):
            arrived(full.at[rr, cols(peer(s))], sl[i])

    sx = [slot() for _ in range(13)]
    sd = [slot() for _ in range(13)]
    x_sends = plane_first(x_in, x_all, sx)

    def wz(k, p, sl, device):
        a, b = w13.at[cols(p), cols(k, 2 * LANE)], w2.at[cols(k), cols(p)]
        return (rcopy(a, a, wz_send.at[sl, p, 0], wz_recv.at[sl, p, 0], (device, t)),
                rcopy(b, b, wz_send.at[sl, p, 1], wz_recv.at[sl, p, 1], (device, t)))

    def wz_own(p):
        @pl.when(is_end)
        def _():
            for c in wz(c_end, p, 3, inner):
                c.start()

        @pl.when(is_mid)
        def _():
            for c in wz(c_mid, p, 0, outer) + wz(c_mid, p, 4, inner):
                c.start()

    for c in loc[:3]:
        c.wait()
    wz_own(t)
    for s in (1, 2, 4, 3, 5, 6, 7):
        p = peer(s)
        a, b, c, d = w_slots[s]
        arrived(w13.at[cols(p), cols(2 * z)], a)
        arrived(w13.at[cols(p), cols(2 * z + 1)], b)
        arrived(w2.at[cols(z), cols(p)], c)
        arrived(gain_all.at[:, cols(p)], d)
        wz_own(p)

    x_sends += plane_forward(x_all, sx)
    plane_first(dy_in, dy_all, sd)

    def each_block(fn):
        lax.fori_loop(0, N_T, lambda p, c: (fn(p), c)[1], 0)

    def wz_wait(k, p, sl):
        for c in wz(k, p, sl, inner):
            c.wait_recv()

    def hop_one(p):
        wz_wait(c_end, p, 3)
        for c in wz(c_end, p, 5, inner):
            c.start()
        wz_wait(c_mid2, p, 4)
        for c in wz(c_mid2, p, 1, outer):
            c.start()

    def hop_two(p):
        wz_wait(c_end2, p, 5)
        for c in wz(c_end2, p, 2, outer):
            c.start()

    @pl.when(is_mid)
    def _():
        each_block(hop_one)

    x_sends += plane_rest(x_all, sx)
    for c in loc[3:5]:
        c.wait()
    plane_last(x_all, sx)

    def norm(xf):
        d = xf.shape[1]
        mu = jnp.sum(xf, axis=1, keepdims=True) / d
        sq = jnp.sum(xf * xf, axis=1, keepdims=True) / d
        r = lax.rsqrt(sq - mu * mu + LN_EPS)
        return (xf - mu) * r, r

    def norm_tile(i, carry):
        rr = pl.ds(pl.multiple_of(i * rows, rows), rows)
        xhat, _ = norm(x_all[rr, :].astype(F32))
        h_all[rr, :] = (gain_all[0:1, :] * xhat).astype(BF16)
        return carry

    def block(p):
        return pl.ds(pl.multiple_of(p * rows, rows), rows)

    lax.fori_loop(0, N_T, norm_tile, 0)
    x_rows[...] = x_all[block(t), :]
    plane_forward(dy_all, sd)

    @pl.when(is_mid)
    def _():
        each_block(hop_two)

    plane_rest(dy_all, sd)
    loc[5].wait()
    plane_last(dy_all, sd)
    for c in x_sends:
        c.wait_send()

    def piece(p):
        return pl.ds(p * ROWS, ROWS)

    def sum_copy(src, dst, sl, p, device):
        return rcopy(src, dst, sum_send.at[sl, p], sum_recv.at[sl, p], (device, t))

    def from_end(q, k, p):
        return sum_copy(dw.at[k, piece(p)], outs.at[q, piece(p)], q, p, inner)

    def end_send(q, k):
        @pl.when(is_end)
        def _():
            for p in range(PIECES):
                from_end(q, k, p).start()

    def chunk_step(i, carry):
        b = i + (1 - 2 * lax.rem(i, 2)) * (1 - lax.div(i, 2))
        k = low * b + (1 - low) * (3 - b)

        for step, sl in ((0, 0), (2, 1), (3, 2)):
            @pl.when(jnp.logical_and(is_end, i == step))
            def _(sl=sl):
                each_block(lambda p: wz_wait(k, p, sl))

        def tile(j, c):
            rr = block(j)
            uv = dot(h_all[rr, :], w13[:, cols(k, 2 * LANE)])
            da = dot_cols(dy_all[rr, :], w2[cols(k), :])
            u, v = uv[:, :LANE], uv[:, LANE:]
            sig = jax.nn.sigmoid(u)
            swish = u * sig
            a = (swish * v).astype(BF16)
            du = (da * v * sig * (1.0 + u * (1.0 - sig))).astype(BF16)
            dv = (da * swish).astype(BF16)
            act[rr, cols(k)] = a
            duv[rr, cols(2 * k)] = du
            duv[rr, cols(2 * k + 1)] = dv
            act_t[:, rr] = a.T
            duv_t[0:LANE, rr] = du.T
            duv_t[LANE:, rr] = dv.T
            return c

        lax.fori_loop(0, N_T, tile, 0)

        def grad(n, c):
            nn = cols(n, 2 * LANE)
            dw[k, 0:2 * LANE, nn] = dot(duv_t[...], h_all[:, nn])
            dw[k, 2 * LANE:, nn] = dot(act_t[...], dy_all[:, nn])
            return c

        lax.fori_loop(0, dy_all.shape[1] // (2 * LANE), grad, 0)

        @pl.when(i == 0)
        def _():
            end_send(2, c_mid)
        return carry

    lax.fori_loop(0, N_Z, chunk_step, 0)
    end_send(1, c_end2)
    end_send(0, c_mid2)

    def stage0(away, r0, make, base):
        def body(j, c):
            fx, fy = 1 - lax.div(j, 2), 1 - lax.rem(j, 2)
            i = fx + 2 * fy
            away[i] = make(block(pc + fx * flips[1] + fy * flips[2]))
            rcopy(away.at[i], r0.at[i], red_send.at[base + i], red_recv.at[base + i], (z, pc)).start()
            return c
        lax.fori_loop(0, 4, body, 0)

    def stage1(r0, make, base):
        def body(j, c):
            fx, fy = 1 - lax.div(j, 2), 1 - lax.rem(j, 2)
            i = fx + 2 * fy
            rcopy(r0.at[i], r0.at[i], red_send.at[base + i], red_recv.at[base + i], (z, pc)).wait_recv()
            r0[i] += make(block(t + fx * flips[1] + fy * flips[2]))
            return c
        lax.fori_loop(0, 4, body, 0)

    def rsend(src, dst, sl, device):
        c = rcopy(src, dst, red_send.at[sl], red_recv.at[sl], device)
        c.start()
        pending.append(c)

    def rarrived(dst, sl):
        rcopy(dst, dst, red_send.at[sl], red_recv.at[sl], (z, pc)).wait_recv()

    a_half, b_half = pl.ds(0, hr), pl.ds(hr, hr)

    def stage1_send(r0, r1, base):
        rsend(r0.at[3, a_half], r1.at[0], base + 4, (z, px))
        rsend(r0.at[3, b_half], r1.at[1], base + 5, (z, py))
        rsend(r0.at[1, a_half], r1.at[2], base + 6, (z, px))
        rsend(r0.at[2, b_half], r1.at[3], base + 7, (z, py))

    def stage2(r0, r1, r2, base):
        rarrived(r1.at[0], base + 4)
        r0[2, 0:hr] += r1[0]
        rsend(r0.at[2, a_half], r2.at[0], base + 8, (z, py))
        rarrived(r1.at[1], base + 5)
        r0[1, hr:rows] += r1[1]
        rsend(r0.at[1, b_half], r2.at[1], base + 9, (z, px))

    def stage3(r0, r1, base):
        rarrived(r1.at[2], base + 6)
        r0[0, 0:hr] += r1[2]
        rarrived(r1.at[3], base + 7)
        r0[0, hr:rows] += r1[3]

    def stage4(r0, r2, base):
        rarrived(r2.at[0], base + 8)
        r0[0, 0:hr] += r2[0]
        rarrived(r2.at[1], base + 9)
        r0[0, hr:rows] += r2[1]

    def make_m(rr):
        return dot(act[rr, :], w2[...])

    def make_dh(rr):
        return dot_cols(duv[rr, :], w13[...])

    stage0(m_away, m0, make_m, 0)
    stage0(e_away, e0, make_dh, 10)
    stage1(m0, make_m, 0)
    stage1_send(m0, m1, 0)
    stage1(e0, make_dh, 10)
    stage1_send(e0, e1, 10)

    def finish(src, p):
        for s in (6, 7, 2, 4, 3, 5, 1):
            q = peer(s)
            rcopy(src.at[:, cols(q)], dw_out.at[t, piece(p)], fin_send.at[s, p], fin_recv.at[s, p], (z, q)).start()
        pltpu.make_async_copy(src.at[:, cols(t)], dw_out.at[t, piece(p)], fin_send.at[0, p]).start()

    def pass_in(q, k, p):
        @pl.when(is_mid)
        def _():
            ref = outs.at[q, piece(p)]
            sum_copy(ref, ref, q, p, outer).wait_recv()
            outs[q, p * ROWS:(p + 1) * ROWS] += dw[k, p * ROWS:(p + 1) * ROWS]
            sum_copy(ref, ins.at[q, piece(p)], 3 + q, p, inner).start()

    def pass_out(p):
        @pl.when(is_mid)
        def _():
            ref = ins.at[1, piece(p)]
            sum_copy(ref, ref, 4, p, inner).wait_recv()
            ins[1, p * ROWS:(p + 1) * ROWS] += dw[c_end, p * ROWS:(p + 1) * ROWS]
            sum_copy(ref, ref, 5, p, outer).start()

    def last_mid(p):
        @pl.when(is_mid)
        def _():
            a, b = outs.at[2, piece(p)], ins.at[0, piece(p)]
            sum_copy(b, b, 3, p, inner).wait_recv()
            sum_copy(a, a, 2, p, outer).wait_recv()
            rr = slice(p * ROWS, (p + 1) * ROWS)
            outs[2, rr] += ins[0, rr] + dw[c_mid, rr]
            finish(a, p)

    def last_end(p):
        @pl.when(is_end)
        def _():
            a = ins.at[1, piece(p)]
            sum_copy(a, a, 5, p, inner).wait_recv()
            rr = slice(p * ROWS, (p + 1) * ROWS)
            ins[1, rr] += dw[c_end, rr]
            finish(a, p)

    def spread(src, dst, base, local):
        for s in (6, 7, 2, 4, 3, 5, 1):
            q = peer(s)
            rsend(src.at[:, cols(q)], dst.at[block(t), :], base + s - 1, (z, q))
        c = pltpu.make_async_copy(src.at[:, cols(t)], dst.at[block(t), :], local_sem.at[local])
        c.start()
        loc.append(c)

    def make_y():
        stage4(m0, m2, 0)
        y_rows[...] = (x_rows[...].astype(F32) + m0[0]).astype(BF16)
        spread(y_rows, y_out, 20, 6)

    def make_dx():
        stage4(e0, e2, 10)
        xhat, r = norm(x_rows[...].astype(F32))
        d = xhat.shape[1]
        dh = e0[0]
        e = dh * gain_all[0:1, :]
        e_mean = jnp.sum(e, axis=1, keepdims=True) / d
        ex_mean = jnp.sum(e * xhat, axis=1, keepdims=True) / d
        dy_rows = dy_all[block(t), :].astype(F32)
        dx_rows[...] = (dy_rows + r * (e - e_mean - xhat * ex_mean)).astype(BF16)
        dg_rows[...] = jnp.sum((dh * xhat).reshape(rows // 8, 8, d), axis=0)
        spread(dx_rows, dx_out, 27, 7)
        for s in order:
            rsend(dg_rows.at[:, cols(peer(s))], dg_plane.at[s - 1], 34 + s - 1, (z, peer(s)))

    def gain_plane():
        total = dg_rows[:, cols(t)]
        for s in range(1, 8):
            rarrived(dg_plane.at[s - 1], 34 + s - 1)
            total = total + dg_plane[s - 1]
        dg_line[0] = total
        for s in range(1, 4):
            rsend(dg_line.at[0], dg_line.at[s], 40 + s, (lax.rem(z + s, 4), t))

    def gain_line():
        for s in range(1, 4):
            rarrived(dg_line.at[s], 40 + s)
        parts = [dg_line[lax.rem(z - s + 4, 4)] for s in range(4)]
        dg_out[...] = (parts[0] + parts[1]) + (parts[2] + parts[3])

    per = 33.7 / PIECES
    plan = [(90, lambda: stage2(m0, m1, m2, 0)), (101, lambda: stage3(m0, m1, 0)),
            (113, lambda: stage2(e0, e1, e2, 10)), (124, lambda: stage3(e0, e1, 10)),
            (135, make_y), (147, make_dx), (151, gain_plane), (157, gain_line)]
    for p in range(PIECES):
        done = 83 + per * (p + 1)
        plan.append((done, lambda p=p: pass_in(1, c_end2, p)))
        plan.append((done + per + 1, lambda p=p: pass_out(p)))
        plan.append((done + 2 * per + 2, lambda p=p: last_end(p)))
        plan.append((done + 33.7, lambda p=p: pass_in(0, c_mid2, p)))
        plan.append((done + 33.7 + per + 1, lambda p=p: last_mid(p)))
    for _, fn in sorted(plan, key=lambda e: e[0]):
        fn()

    for s in range(1, 8):
        q = peer(s)
        rarrived(y_out.at[block(q), :], 20 + s - 1)
        rarrived(dx_out.at[block(q), :], 27 + s - 1)
        for p in range(PIECES):
            c = rcopy(outs.at[2, piece(p), cols(q)], dw_out.at[q, piece(p)], fin_send.at[s, p], fin_recv.at[s, p], (z, q))
            c.wait_send()
            c.wait_recv()
    for p in range(PIECES):
        pltpu.make_async_copy(outs.at[2, piece(p), cols(t)], dw_out.at[t, piece(p)], fin_send.at[0, p]).wait()
    for c in loc[6:]:
        c.wait()
    skip = set(id(c) for c in x_sends)
    for c in pending:
        if id(c) not in skip:
            c.wait_send()
    for away, r0, base in ((m_away, m0, 0), (e_away, e0, 10)):
        for i in range(4):
            rcopy(away.at[i], r0.at[i], red_send.at[base + i], red_recv.at[base + i], (z, pc)).wait_send()

    def sent(k, p, sl):
        for c in wz(k, p, sl, inner):
            c.wait_send()

    @pl.when(is_end)
    def _():
        each_block(lambda p: sent(c_end, p, 3))
        for q in range(3):
            for p in range(PIECES):
                from_end(q, c_mid, p).wait_send()

    @pl.when(is_mid)
    def _():
        def all_sent(p):
            for sl in (0, 1, 2, 4, 5):
                sent(c_mid, p, sl)
        each_block(all_sent)
        for sl in (3, 4, 5):
            for p in range(PIECES):
                sum_copy(outs.at[0, piece(p)], ins.at[0, piece(p)], sl, p, inner).wait_send()


def place_kernel(y_in, dx_in, dw_in, dg_in, y_out, dx_out, dw1_out, dw3_out, dw2_out, dg_out):
    y_out[...] = y_in[...]
    dx_out[...] = dx_in[...]
    for s in range(N_T):
        at = slice(s * LANE, (s + 1) * LANE)
        dw1_out[:, at] = dw_in[s, 0:LANE].T
        dw3_out[:, at] = dw_in[s, LANE:2 * LANE].T
        dw2_out[at, :] = dw_in[s, 2 * LANE:]
    dg_out[...] = jnp.sum(dg_in[...], axis=0, keepdims=True)


def solution(mesh):
    def local_step(x_blk, dy_blk, gain_blk, w1_blk, w3_blk, w2_blk):
        tokens, lane = x_blk.shape
        d = lane * N_T
        f = w1_blk.shape[1] // N_T * N_Z
        rows = tokens // N_T
        gain8 = jnp.broadcast_to(gain_blk[None, :], (8, lane))
        any_spec = pl.BlockSpec(memory_space=pl.ANY)
        vmem = pl.BlockSpec(memory_space=pltpu.VMEM)
        s = jax.ShapeDtypeStruct
        V = pltpu.VMEM
        dma = pltpu.SemaphoreType.DMA
        red = [V((4, rows, d), F32), V((4, rows, d), F32), V((4, rows // 2, d), F32), V((2, rows // 2, d), F32)]
        y, dx, dw, dg = pl.pallas_call(
            step_kernel,
            out_shape=(s((tokens, lane), BF16), s((tokens, lane), BF16), s((N_T, 384, lane), F32), s((8, lane), F32)),
            in_specs=[any_spec] * 6,
            out_specs=[any_spec] * 3 + [vmem],
            scratch_shapes=[
                V((tokens, d), BF16), V((tokens, d), BF16), V((tokens, d), BF16), V((8, d), F32),
                V((d, 2 * f), BF16), V((f, d), BF16), V((tokens, f), BF16), V((lane, tokens), BF16),
                V((2 * lane, tokens), BF16), V((N_Z, 384, d), F32)] + red + red + [
                V((3, 384, d), F32), V((2, 384, d), F32),
                V((rows, d), BF16), V((rows, d), BF16), V((rows, d), BF16), V((8, d), F32),
                V((7, 8, lane), F32), V((4, 8, lane), F32),
                dma((N_PLANE,)), dma((N_PLANE,)), dma((6, N_T, 2)), dma((6, N_T, 2)),
                dma((6, PIECES)), dma((6, PIECES)), dma((8, PIECES)), dma((8, PIECES)),
                dma((N_RED,)), dma((N_RED,)), dma((8,))],
            compiler_params=pltpu.CompilerParams(has_side_effects=True, vmem_limit_bytes=67043328),
            name="step",
        )(x_blk, dy_blk, gain8, w1_blk, w3_blk, w2_blk)
        f_z = w1_blk.shape[1]
        y, dx, dw1, dw3, dw2, dg = pl.pallas_call(
            place_kernel,
            out_shape=(s((tokens, lane), BF16), s((tokens, lane), BF16), s((lane, f_z), F32), s((lane, f_z), F32),
                       s((f_z, lane), F32), s((1, lane), F32)),
            in_specs=[vmem] * 4, out_specs=[vmem] * 6, name="place",
        )(y, dx, dw, dg)
        return y, dx, dw1, dw3, dw2, dg[0]

    return jax.shard_map(
        local_step, mesh=mesh,
        in_specs=(P("ty", "tx"), P("ty", "tx"), P("tx"), P("tx", "ty"), P("tx", "ty"), P("ty", "tx")),
        out_specs=(P("ty", "tx"), P("ty", "tx"), P("tx", "ty"), P("tx", "ty"), P("ty", "tx"), P("tx")),
        check_vma=False)
```

```python
import jax
import jax.numpy as jnp
from jax import lax
from jax.experimental import pallas as pl
from jax.experimental.pallas import tpu as pltpu
from jax.sharding import PartitionSpec as P

LN_EPS = 1e-6
F32 = jnp.float32
BF16 = jnp.bfloat16
MESH = pl.DeviceIdType.MESH
LANE = 128
N_T = 8
N_Z = 4
PIECES = 6
ROWS = 384 // PIECES
PIECE_ORDER = tuple(range(PIECES * 2 // 3, PIECES)) + tuple(range(PIECES * 2 // 3))


def cols(k, width=LANE):
    return pl.ds(pl.multiple_of(k * width, width), width)


def dot(a, b):
    return jnp.dot(a, b, preferred_element_type=F32)


def dot_cols(a, b):
    return lax.dot_general(a, b, (((1,), (1,)), ((), ())), preferred_element_type=F32)


N_PLANE = 28 + 26
N_RED = 20 + 21 + 3
N_SUM = 6 * PIECES


def step_kernel(x_in, dy_in, g_in, w1_in, w3_in, w2_in,
                y_out, dx_out, dw_out, dg_out,
                x_all, h_all, dy_all, gain_all, w13, w2, act, act_t, duv_t, dw, uv_all,
                m_away, m0, m1, m2, e0, e1, e2, outs, ins,
                x_rows, y_rows, dx_rows, dg_rows, dg_plane, dg_line,
                send_sem, recv_sem, wz_send, wz_recv, sum_send, sum_recv, fin_send, fin_recv,
                red_send, red_recv, local_sem):
    z = lax.axis_index("ty")
    t = lax.axis_index("tx")
    core = lax.rem(t, 2)
    xbit = lax.rem(lax.div(t, 2), 2)
    ybit = lax.div(t, 4)
    flips = (1 - 2 * core, 2 - 4 * xbit, 4 - 8 * ybit)
    duv = x_all
    e_away = uv_all.at[pl.ds(4, 4)]

    def peer(s):
        out = t
        for bit in range(3):
            if s >> bit & 1:
                out = out + flips[bit]
        return out

    px, py, pd, pc = peer(2), peer(4), peer(6), peer(1)
    order = (2, 4, 3, 5, 6, 7, 1)
    tokens = x_all.shape[0]
    half = tokens // 2
    rows = tokens // N_T
    hr = rows // 2

    low = lax.div(3 - z, 2)
    is_end = jnp.logical_or(z == 0, z == 3)
    is_mid = jnp.logical_or(z == 1, z == 2)
    c_end = 3 - 3 * low
    c_mid = 2 - low
    c_mid2 = 3 - c_mid
    c_end2 = 3 - c_end
    inner = z + 2 * low - 1
    outer = z - 2 * low + 1

    def rcopy(src, dst, ssem, rsem, device):
        return pltpu.make_async_remote_copy(src_ref=src, dst_ref=dst, send_sem=ssem, recv_sem=rsem,
                                            device_id=device, device_id_type=MESH)

    count = [0]

    def slot():
        count[0] += 1
        return count[0] - 1

    pending = []

    def send(src, dst, sl, device):
        c = rcopy(src, dst, send_sem.at[sl], recv_sem.at[sl], device)
        c.start()
        pending.append(c)
        return c

    def arrived(dst, sl):
        rcopy(dst, dst, send_sem.at[sl], recv_sem.at[sl], (z, pc)).wait_recv()

    loc = [
        pltpu.make_async_copy(w1_in.at[:, cols(t)], w13.at[cols(t), cols(2 * z)], local_sem.at[0]),
        pltpu.make_async_copy(w3_in.at[:, cols(t)], w13.at[cols(t), cols(2 * z + 1)], local_sem.at[1]),
        pltpu.make_async_copy(w2_in.at[cols(t), :], w2.at[cols(z), cols(t)], local_sem.at[2]),
        pltpu.make_async_copy(g_in, gain_all.at[:, cols(t)], local_sem.at[3]),
        pltpu.make_async_copy(x_in, x_all.at[:, cols(t)], local_sem.at[4]),
        pltpu.make_async_copy(dy_in, dy_all.at[:, cols(t)], local_sem.at[5]),
    ]
    for c in loc:
        c.start()
    barrier = pltpu.get_barrier_semaphore()
    for s in order:
        pl.semaphore_signal(barrier, inc=1, device_id=(z, peer(s)), device_id_type=MESH)
    for s in range(1, N_Z):
        pl.semaphore_signal(barrier, inc=1, device_id=(lax.rem(z + s, N_Z), t), device_id_type=MESH)
    pl.semaphore_wait(barrier, N_T - 1 + N_Z - 1)

    w_slots = {}
    for s in order:
        p = peer(s)
        w_slots[s] = [slot() for _ in range(4)]
        a, b, c, d = w_slots[s]
        send(w1_in.at[:, cols(p)], w13.at[cols(t), cols(2 * z)], a, (z, p))
        send(w3_in.at[:, cols(p)], w13.at[cols(t), cols(2 * z + 1)], b, (z, p))
        send(w2_in.at[cols(p), :], w2.at[cols(z), cols(t)], c, (z, p))
        send(g_in, gain_all.at[:, cols(t)], d, (z, p))

    lo, hi = pl.ds(0, half), pl.ds(half, half)

    def plane_first(src, full, sl):
        return [send(src.at[lo], full.at[lo, cols(t)], sl[0], (z, px)),
                send(src.at[hi], full.at[hi, cols(t)], sl[2], (z, py)),
                send(src.at[hi], full.at[hi, cols(t)], sl[1], (z, px)),
                send(src.at[lo], full.at[lo, cols(t)], sl[3], (z, py)),
                send(src, full.at[:, cols(t)], sl[4], (z, pc))]

    def forward(ref, sl, device):
        return send(ref, ref, sl, (z, device))

    def plane_forward(full, sl):
        a, b = full.at[lo, cols(px)], full.at[hi, cols(py)]
        arrived(a, sl[0])
        out = [forward(a, sl[5], py), forward(a, sl[7], pc)]
        arrived(b, sl[2])
        return out + [forward(b, sl[6], px), forward(b, sl[9], pc)]

    def plane_rest(full, sl, first, n=2):
        out = []
        for rr, p, i, o in ((hi, px, 1, 8), (lo, py, 3, 10), (lo, pd, 5, 11), (hi, pd, 6, 12))[first:first + n]:
            ref = full.at[rr, cols(p)]
            arrived(ref, sl[i])
            out.append(forward(ref, sl[o], pc))
        return out

    def plane_last(full, sl):
        arrived(full.at[:, cols(pc)], sl[4])
        for rr, s, i in ((lo, 3, 7), (hi, 3, 8), (hi, 5, 9), (lo, 5, 10), (lo, 7, 11), (hi, 7, 12)):
            arrived(full.at[rr, cols(peer(s))], sl[i])

    sx = [slot() for _ in range(13)]
    sd = [slot() for _ in range(13)]
    x_sends = plane_first(x_in, x_all, sx)

    def wz(k, p, sl, device):
        a, b = w13.at[cols(p), cols(k, 2 * LANE)], w2.at[cols(k), cols(p)]
        return (rcopy(a, a, wz_send.at[sl, p, 0], wz_recv.at[sl, p, 0], (device, t)),
                rcopy(b, b, wz_send.at[sl, p, 1], wz_recv.at[sl, p, 1], (device, t)))

    def wz_own(p):
        @pl.when(is_end)
        def _():
            for c in wz(c_end, p, 3, inner):
                c.start()

        @pl.when(is_mid)
        def _():
            for c in wz(c_mid, p, 0, outer) + wz(c_mid, p, 4, inner):
                c.start()

    for c in loc[:3]:
        c.wait()
    wz_own(t)
    for s in (1, 2, 4, 3, 5, 6, 7):
        p = peer(s)
        a, b, c, d = w_slots[s]
        arrived(w13.at[cols(p), cols(2 * z)], a)
        arrived(w13.at[cols(p), cols(2 * z + 1)], b)
        arrived(w2.at[cols(z), cols(p)], c)
        arrived(gain_all.at[:, cols(p)], d)
        wz_own(p)

    x_sends += plane_forward(x_all, sx)
    plane_first(dy_in, dy_all, sd)

    def each_block(fn):
        lax.fori_loop(0, N_T, lambda p, c: (fn(p), c)[1], 0)

    def wz_wait(k, p, sl):
        for c in wz(k, p, sl, inner):
            c.wait_recv()

    def hop_one(p):
        wz_wait(c_end, p, 3)
        for c in wz(c_end, p, 5, inner):
            c.start()
        wz_wait(c_mid2, p, 4)
        for c in wz(c_mid2, p, 1, outer):
            c.start()

    def hop_two(p):
        wz_wait(c_end2, p, 5)
        for c in wz(c_end2, p, 2, outer):
            c.start()

    @pl.when(is_mid)
    def _():
        each_block(hop_one)

    x_sends += plane_rest(x_all, sx, 0, 4)
    for c in loc[3:5]:
        c.wait()
    plane_last(x_all, sx)

    def norm(xf):
        d = xf.shape[1]
        mu = jnp.sum(xf, axis=1, keepdims=True) / d
        sq = jnp.sum(xf * xf, axis=1, keepdims=True) / d
        r = lax.rsqrt(sq - mu * mu + LN_EPS)
        return (xf - mu) * r, r

    def norm_tile(i, carry):
        rr = pl.ds(pl.multiple_of(i * rows, rows), rows)
        xhat, _ = norm(x_all[rr, :].astype(F32))
        h_all[rr, :] = (gain_all[0:1, :] * xhat).astype(BF16)
        return carry

    def block(p):
        return pl.ds(pl.multiple_of(p * rows, rows), rows)

    def piece(p):
        return pl.ds(p * ROWS, ROWS)

    def sum_copy(src, dst, sl, p, device):
        return rcopy(src, dst, sum_send.at[sl, p], sum_recv.at[sl, p], (device, t))

    def from_end(q, k, p):
        return sum_copy(dw.at[k, piece(p)], outs.at[q, piece(p)], q, p, inner)

    def end_send(q, k, pieces):
        @pl.when(is_end)
        def _():
            for p in pieces:
                from_end(q, k, p).start()

    def uv_tile(i, j):
        return 2 * i + lax.div(j, 4), cols(lax.rem(j, 4), 2 * LANE)

    def forward_chunk(i, k, sl):
        if sl is not None:
            @pl.when(is_end)
            def _():
                each_block(lambda p: wz_wait(k, p, sl))

        def tile(j, c):
            rr = block(j)
            uv = dot(h_all[rr, :], w13[:, cols(k, 2 * LANE)])
            at, cc = uv_tile(i, j)
            uv_all[at, :, cc] = uv
            u, v = uv[:, :LANE], uv[:, LANE:]
            act[rr, cols(k)] = (u * jax.nn.sigmoid(u) * v).astype(BF16)
            return c

        lax.fori_loop(0, N_T, tile, 0)

    def turn_act(k):
        def tile(j, c):
            act_t[:, block(j)] = act[block(j), cols(k)].T
            return c
        lax.fori_loop(0, N_T, tile, 0)

    n_cols = dy_all.shape[1] // (2 * LANE)

    def grad_down(k):
        def grad(n, c):
            nn = cols(n, 2 * LANE)
            dw[k, 2 * LANE:, nn] = dot(act_t[...], dy_all[:, nn])
            return c
        lax.fori_loop(0, n_cols, grad, 0)

    def backward_chunk(i, k):
        def tile(j, c):
            rr = block(j)
            da = dot_cols(dy_all[rr, :], w2[cols(k), :])
            at, cc = uv_tile(i, j)
            uv = uv_all[at, :, cc]
            u, v = uv[:, :LANE], uv[:, LANE:]
            sig = jax.nn.sigmoid(u)
            du = (da * v * sig * (1.0 + u * (1.0 - sig))).astype(BF16)
            dv = (da * (u * sig)).astype(BF16)
            duv[rr, cols(2 * k)] = du
            duv[rr, cols(2 * k + 1)] = dv
            duv_t[0:LANE, rr] = du.T
            duv_t[LANE:, rr] = dv.T
            return c

        lax.fori_loop(0, N_T, tile, 0)

        def grad(n, c):
            nn = cols(n, 2 * LANE)
            dw[k, 0:2 * LANE, nn] = dot(duv_t[...], h_all[:, nn])
            return c

        lax.fori_loop(0, n_cols, grad, 0)

    lax.fori_loop(0, N_T, norm_tile, 0)
    x_rows[...] = x_all[block(t), :]
    forward_chunk(0, c_mid, 0)
    plane_forward(dy_all, sd)

    @pl.when(is_mid)
    def _():
        each_block(hop_two)

    forward_chunk(1, c_end, None)
    turn_act(c_mid)
    plane_rest(dy_all, sd, 0)
    forward_chunk(2, c_mid2, 1)
    plane_rest(dy_all, sd, 2)
    loc[5].wait()
    plane_last(dy_all, sd)
    for c in x_sends:
        c.wait_send()
    grad_down(c_mid)
    end_send(2, c_mid, PIECE_ORDER[:2])
    backward_chunk(0, c_mid)
    end_send(2, c_mid, PIECE_ORDER[2:])

    def stage0(away, r0, make, base):
        def body(j, c):
            fx, fy = 1 - lax.div(j, 2), 1 - lax.rem(j, 2)
            i = fx + 2 * fy
            away[i] = make(block(pc + fx * flips[1] + fy * flips[2]))
            rcopy(away.at[i], r0.at[i], red_send.at[base + i], red_recv.at[base + i], (z, pc)).start()
            return c
        lax.fori_loop(0, 4, body, 0)

    def rsend(src, dst, sl, device):
        c = rcopy(src, dst, red_send.at[sl], red_recv.at[sl], device)
        c.start()
        pending.append(c)

    def rarrived(dst, sl):
        rcopy(dst, dst, red_send.at[sl], red_recv.at[sl], (z, pc)).wait_recv()

    a_half, b_half = pl.ds(0, hr), pl.ds(hr, hr)

    def stage1(r0, r1, make, base):
        for i in (3, 1, 2, 0):
            rcopy(r0.at[i], r0.at[i], red_send.at[base + i], red_recv.at[base + i], (z, pc)).wait_recv()
            r0[i] += make(block((t, px, py, pd)[i]))
            if i == 3:
                rsend(r0.at[3, a_half], r1.at[0], base + 4, (z, px))
                rsend(r0.at[3, b_half], r1.at[1], base + 5, (z, py))
            if i == 1:
                rsend(r0.at[1, a_half], r1.at[2], base + 6, (z, px))
            if i == 2:
                rsend(r0.at[2, b_half], r1.at[3], base + 7, (z, py))

    def stage2(r0, r1, r2, base):
        rarrived(r1.at[0], base + 4)
        r0[2, 0:hr] += r1[0]
        rsend(r0.at[2, a_half], r2.at[0], base + 8, (z, py))
        rarrived(r1.at[1], base + 5)
        r0[1, hr:rows] += r1[1]
        rsend(r0.at[1, b_half], r2.at[1], base + 9, (z, px))

    def stage3(r0, r1, base):
        rarrived(r1.at[2], base + 6)
        r0[0, 0:hr] += r1[2]
        rarrived(r1.at[3], base + 7)
        r0[0, hr:rows] += r1[3]

    def stage4(r0, r2, base):
        rarrived(r2.at[0], base + 8)
        r0[0, 0:hr] += r2[0]
        rarrived(r2.at[1], base + 9)
        r0[0, hr:rows] += r2[1]

    def make_m(rr):
        return dot(act[rr, :], w2[...])

    def make_dh(rr):
        return dot_cols(duv[rr, :], w13[...])

    def rest_of_chunk(i, k):
        turn_act(k)
        grad_down(k)
        backward_chunk(i, k)

    forward_chunk(3, c_end2, 2)
    stage0(m_away, m0, make_m, 0)
    stage1(m0, m1, make_m, 0)
    rest_of_chunk(3, c_end2)
    end_send(1, c_end2, PIECE_ORDER)
    rest_of_chunk(1, c_end)
    stage2(m0, m1, m2, 0)
    rest_of_chunk(2, c_mid2)
    end_send(0, c_mid2, PIECE_ORDER)
    stage0(e_away, e0, make_dh, 10)
    stage1(e0, e1, make_dh, 10)

    def finish(src, p):
        for s in (6, 7, 2, 4, 3, 5, 1):
            q = peer(s)
            rcopy(src.at[:, cols(q)], dw_out.at[t, piece(p)], fin_send.at[s, p], fin_recv.at[s, p], (z, q)).start()
        pltpu.make_async_copy(src.at[:, cols(t)], dw_out.at[t, piece(p)], fin_send.at[0, p]).start()

    def pass_in(q, k, p):
        @pl.when(is_mid)
        def _():
            ref = outs.at[q, piece(p)]
            sum_copy(ref, ref, q, p, outer).wait_recv()
            outs[q, p * ROWS:(p + 1) * ROWS] += dw[k, p * ROWS:(p + 1) * ROWS]
            sum_copy(ref, ins.at[q, piece(p)], 3 + q, p, inner).start()

    def pass_out(p):
        @pl.when(is_mid)
        def _():
            ref = ins.at[1, piece(p)]
            sum_copy(ref, ref, 4, p, inner).wait_recv()
            ins[1, p * ROWS:(p + 1) * ROWS] += dw[c_end, p * ROWS:(p + 1) * ROWS]
            sum_copy(ref, ref, 5, p, outer).start()

    def last_mid(p):
        @pl.when(is_mid)
        def _():
            a, b = outs.at[2, piece(p)], ins.at[0, piece(p)]
            sum_copy(b, b, 3, p, inner).wait_recv()
            sum_copy(a, a, 2, p, outer).wait_recv()
            rr = slice(p * ROWS, (p + 1) * ROWS)
            outs[2, rr] += ins[0, rr] + dw[c_mid, rr]
            finish(a, p)

    def last_end(p):
        @pl.when(is_end)
        def _():
            a = ins.at[1, piece(p)]
            sum_copy(a, a, 5, p, inner).wait_recv()
            rr = slice(p * ROWS, (p + 1) * ROWS)
            ins[1, rr] += dw[c_end, rr]
            finish(a, p)

    def spread(src, dst, base, local):
        for s in (6, 7, 2, 4, 3, 5, 1):
            q = peer(s)
            rsend(src.at[:, cols(q)], dst.at[block(t), :], base + s - 1, (z, q))
        c = pltpu.make_async_copy(src.at[:, cols(t)], dst.at[block(t), :], local_sem.at[local])
        c.start()
        loc.append(c)

    def make_y():
        stage4(m0, m2, 0)
        y_rows[...] = (x_rows[...].astype(F32) + m0[0]).astype(BF16)
        spread(y_rows, y_out, 20, 6)

    def make_dx():
        stage4(e0, e2, 10)
        xhat, r = norm(x_rows[...].astype(F32))
        d = xhat.shape[1]
        dh = e0[0]
        e = dh * gain_all[0:1, :]
        e_mean = jnp.sum(e, axis=1, keepdims=True) / d
        ex_mean = jnp.sum(e * xhat, axis=1, keepdims=True) / d
        dy_rows = dy_all[block(t), :].astype(F32)
        dx_rows[...] = (dy_rows + r * (e - e_mean - xhat * ex_mean)).astype(BF16)
        dg_rows[...] = jnp.sum((dh * xhat).reshape(rows // 8, 8, d), axis=0)
        for s in order:
            rsend(dg_rows.at[:, cols(peer(s))], dg_plane.at[s - 1], 34 + s - 1, (z, peer(s)))
        spread(dx_rows, dx_out, 27, 7)

    def gain_plane():
        total = dg_rows[:, cols(t)]
        for s in range(1, 8):
            rarrived(dg_plane.at[s - 1], 34 + s - 1)
            total = total + dg_plane[s - 1]
        dg_line[0] = total
        for s in range(1, 4):
            rsend(dg_line.at[0], dg_line.at[s], 40 + s, (lax.rem(z + s, 4), t))

    def gain_line():
        for s in range(1, 4):
            rarrived(dg_line.at[s], 40 + s)
        parts = [dg_line[lax.rem(z - s + 4, 4)] for s in range(4)]
        dg_out[...] = (parts[0] + parts[1]) + (parts[2] + parts[3])

    per = 33.7 / PIECES
    plan = [(86, lambda: stage3(m0, m1, 0)), (97, make_y),
            (111, lambda: stage2(e0, e1, e2, 10)), (122, lambda: stage3(e0, e1, 10)),
            (135, make_dx), (143, gain_plane), (157, gain_line)]
    for n, p in enumerate(PIECE_ORDER):
        done = 88 + per * (n + 1)
        plan.append((done, lambda p=p: pass_in(1, c_end2, p)))
        plan.append((done + per + 1, lambda p=p: pass_out(p)))
        plan.append((done + 2 * per + 2, lambda p=p: last_end(p)))
        plan.append((done + 33.7, lambda p=p: pass_in(0, c_mid2, p)))
        plan.append((done + 33.7 + per + 1, lambda p=p: last_mid(p)))
    for _, fn in sorted(plan, key=lambda e: e[0]):
        fn()

    for s in range(1, 8):
        q = peer(s)
        rarrived(y_out.at[block(q), :], 20 + s - 1)
        rarrived(dx_out.at[block(q), :], 27 + s - 1)
        for p in range(PIECES):
            c = rcopy(outs.at[2, piece(p), cols(q)], dw_out.at[q, piece(p)], fin_send.at[s, p], fin_recv.at[s, p], (z, q))
            c.wait_send()
            c.wait_recv()
    for p in range(PIECES):
        pltpu.make_async_copy(outs.at[2, piece(p), cols(t)], dw_out.at[t, piece(p)], fin_send.at[0, p]).wait()
    for c in loc[6:]:
        c.wait()
    skip = set(id(c) for c in x_sends)
    for c in pending:
        if id(c) not in skip:
            c.wait_send()
    for away, r0, base in ((m_away, m0, 0), (e_away, e0, 10)):
        for i in range(4):
            rcopy(away.at[i], r0.at[i], red_send.at[base + i], red_recv.at[base + i], (z, pc)).wait_send()

    def sent(k, p, sl):
        for c in wz(k, p, sl, inner):
            c.wait_send()

    @pl.when(is_end)
    def _():
        each_block(lambda p: sent(c_end, p, 3))
        for q in range(3):
            for p in range(PIECES):
                from_end(q, c_mid, p).wait_send()

    @pl.when(is_mid)
    def _():
        def all_sent(p):
            for sl in (0, 1, 2, 4, 5):
                sent(c_mid, p, sl)
        each_block(all_sent)
        for sl in (3, 4, 5):
            for p in range(PIECES):
                sum_copy(outs.at[0, piece(p)], ins.at[0, piece(p)], sl, p, inner).wait_send()


def place_kernel(y_in, dx_in, dw_in, dg_in, y_out, dx_out, dw1_out, dw3_out, dw2_out, dg_out):
    y_out[...] = y_in[...]
    dx_out[...] = dx_in[...]
    for s in range(N_T):
        at = slice(s * LANE, (s + 1) * LANE)
        dw1_out[:, at] = dw_in[s, 0:LANE].T
        dw3_out[:, at] = dw_in[s, LANE:2 * LANE].T
        dw2_out[at, :] = dw_in[s, 2 * LANE:]
    dg_out[...] = jnp.sum(dg_in[...], axis=0, keepdims=True)


def solution(mesh):
    def local_step(x_blk, dy_blk, gain_blk, w1_blk, w3_blk, w2_blk):
        tokens, lane = x_blk.shape
        d = lane * N_T
        f = w1_blk.shape[1] // N_T * N_Z
        rows = tokens // N_T
        any_spec = pl.BlockSpec(memory_space=pl.ANY)
        vmem = pl.BlockSpec(memory_space=pltpu.VMEM)
        s = jax.ShapeDtypeStruct
        V = pltpu.VMEM
        dma = pltpu.SemaphoreType.DMA
        red = [V((4, rows, d), F32), V((4, rows, d), F32), V((4, rows // 2, d), F32), V((2, rows // 2, d), F32)]
        y, dx, dw, dg = pl.pallas_call(
            step_kernel,
            out_shape=(s((tokens, lane), BF16), s((tokens, lane), BF16), s((N_T, 384, lane), F32), s((8, lane), F32)),
            in_specs=[any_spec] * 6,
            out_specs=[any_spec] * 3 + [vmem],
            scratch_shapes=[
                V((tokens, d), BF16), V((tokens, d), BF16), V((tokens, d), BF16), V((1, d), F32),
                V((d, 2 * f), BF16), V((f, d), BF16), V((tokens, f), BF16), V((lane, tokens), BF16),
                V((2 * lane, tokens), BF16), V((N_Z, 384, d), F32), V((N_T, rows, d), F32)] + red + red[1:] + [
                V((3, 384, d), F32), V((2, 384, d), F32),
                V((rows, d), BF16), V((rows, d), BF16), V((rows, d), BF16), V((8, d), F32),
                V((7, 8, lane), F32), V((4, 8, lane), F32),
                dma((N_PLANE,)), dma((N_PLANE,)), dma((6, N_T, 2)), dma((6, N_T, 2)),
                dma((6, PIECES)), dma((6, PIECES)), dma((8, PIECES)), dma((8, PIECES)),
                dma((N_RED,)), dma((N_RED,)), dma((8,))],
            compiler_params=pltpu.CompilerParams(collective_id=0, has_side_effects=True, vmem_limit_bytes=67043328),
            name="step",
        )(x_blk, dy_blk, gain_blk[None, :], w1_blk, w3_blk, w2_blk)
        f_z = w1_blk.shape[1]
        y, dx, dw1, dw3, dw2, dg = pl.pallas_call(
            place_kernel,
            out_shape=(s((tokens, lane), BF16), s((tokens, lane), BF16), s((lane, f_z), F32), s((lane, f_z), F32),
                       s((f_z, lane), F32), s((1, lane), F32)),
            in_specs=[vmem] * 4, out_specs=[vmem] * 6, name="place",
        )(y, dx, dw, dg)
        return y, dx, dw1, dw3, dw2, dg[0]

    return jax.shard_map(
        local_step, mesh=mesh,
        in_specs=(P("ty", "tx"), P("ty", "tx"), P("tx"), P("tx", "ty"), P("tx", "ty"), P("ty", "tx")),
        out_specs=(P("ty", "tx"), P("ty", "tx"), P("tx", "ty"), P("tx", "ty"), P("ty", "tx"), P("tx")),
        check_vma=False)
```

```python
import jax
import jax.numpy as jnp
from jax import lax
from jax.experimental import pallas as pl
from jax.experimental.pallas import tpu as pltpu
from jax.sharding import PartitionSpec as P

LN_EPS = 1e-6
F32 = jnp.float32
BF16 = jnp.bfloat16
MESH = pl.DeviceIdType.MESH
LANE = 128
N_T = 8
N_Z = 4
PIECES = 6
ROWS = 384 // PIECES
PIECE_ORDER = tuple(range(PIECES * 2 // 3, PIECES)) + tuple(range(PIECES * 2 // 3))


def cols(k, width=LANE):
    return pl.ds(pl.multiple_of(k * width, width), width)


def dot(a, b):
    return jnp.dot(a, b, preferred_element_type=F32)


def dot_cols(a, b):
    return lax.dot_general(a, b, (((1,), (1,)), ((), ())), preferred_element_type=F32)


def step_kernel(x_in, dy_in, g_in, w1_in, w3_in, w2_in,
                y_out, dx_out, dw_out, dg_out,
                x_all, h_all, dy_all, gain_all, w13, w2, act, act_t, duv_t, dw, uv_all,
                m_away, m0, m1, m2, e0, e1, e2, outs, ins,
                x_rows, y_rows, dx_rows, dg_rows, dg_plane, dg_line,
                w_send, w_recv, g_recv, in_send, in_recv, wz_send, wz_end, wz_mid, sum_send, sum_recv,
                fin_sem, red_send, red_recv, local_sem):
    z = lax.axis_index("ty")
    t = lax.axis_index("tx")
    core = lax.rem(t, 2)
    xbit = lax.rem(lax.div(t, 2), 2)
    ybit = lax.div(t, 4)
    flips = (1 - 2 * core, 2 - 4 * xbit, 4 - 8 * ybit)
    duv = x_all
    e_away = uv_all.at[pl.ds(4, 4)]

    def peer(s):
        out = t
        for bit in range(3):
            if s >> bit & 1:
                out = out + flips[bit]
        return out

    px, py, pd, pc = peer(2), peer(4), peer(6), peer(1)
    order = (2, 4, 3, 5, 6, 7, 1)
    tokens = x_all.shape[0]
    half = tokens // 2
    rows = tokens // N_T
    hr = rows // 2

    low = lax.div(3 - z, 2)
    is_end = jnp.logical_or(z == 0, z == 3)
    is_mid = jnp.logical_or(z == 1, z == 2)
    c_end = 3 - 3 * low
    c_mid = 2 - low
    c_mid2 = 3 - c_mid
    c_end2 = 3 - c_end
    inner = z + 2 * low - 1
    outer = z - 2 * low + 1

    def rcopy(src, dst, ssem, rsem, device):
        return pltpu.make_async_remote_copy(src_ref=src, dst_ref=dst, send_sem=ssem, recv_sem=rsem,
                                            device_id=device, device_id_type=MESH)

    def wait_sent(ref, sem):
        rcopy(ref, ref, sem, sem, (z, pc)).wait_send()

    def wait_in(ref, sem):
        rcopy(ref, ref, sem, sem, (z, pc)).wait_recv()

    loc = [
        pltpu.make_async_copy(w1_in.at[:, cols(t)], w13.at[cols(t), cols(2 * z)], local_sem.at[0]),
        pltpu.make_async_copy(w3_in.at[:, cols(t)], w13.at[cols(t), cols(2 * z + 1)], local_sem.at[1]),
        pltpu.make_async_copy(w2_in.at[cols(t), :], w2.at[cols(z), cols(t)], local_sem.at[2]),
        pltpu.make_async_copy(g_in, gain_all.at[:, cols(t)], local_sem.at[3]),
        pltpu.make_async_copy(x_in, x_all.at[:, cols(t)], local_sem.at[4]),
        pltpu.make_async_copy(dy_in, dy_all.at[:, cols(t)], local_sem.at[5]),
    ]
    for c in loc:
        c.start()
    barrier = pltpu.get_barrier_semaphore()
    for s in order:
        pl.semaphore_signal(barrier, inc=1, device_id=(z, peer(s)), device_id_type=MESH)
    for s in range(1, N_Z):
        pl.semaphore_signal(barrier, inc=1, device_id=(lax.rem(z + s, N_Z), t), device_id_type=MESH)
    pl.semaphore_wait(barrier, N_T - 1 + N_Z - 1)

    for s in order:
        p = peer(s)
        rcopy(w1_in.at[:, cols(p)], w13.at[cols(t), cols(2 * z)], w_send.at[0], w_recv.at[s, 0], (z, p)).start()
        rcopy(w3_in.at[:, cols(p)], w13.at[cols(t), cols(2 * z + 1)], w_send.at[1], w_recv.at[s, 0], (z, p)).start()
        rcopy(w2_in.at[cols(p), :], w2.at[cols(z), cols(t)], w_send.at[2], w_recv.at[s, 1], (z, p)).start()
        rcopy(g_in, gain_all.at[:, cols(t)], w_send.at[3], g_recv.at[0], (z, p)).start()

    lo, hi = pl.ds(0, half), pl.ds(half, half)

    def move(n, src, dst, i, device):
        rcopy(src, dst, in_send.at[n], in_recv.at[n, i], (z, device)).start()

    def plane_first(n, src, full):
        move(n, src.at[lo], full.at[lo, cols(t)], 0, px)
        move(n, src.at[hi], full.at[hi, cols(t)], 2, py)
        move(n, src.at[hi], full.at[hi, cols(t)], 1, px)
        move(n, src.at[lo], full.at[lo, cols(t)], 3, py)
        move(n, src, full.at[:, cols(t)], 6, pc)

    def plane_forward(n, full):
        a, b = full.at[lo, cols(px)], full.at[hi, cols(py)]
        wait_in(a, in_recv.at[n, 0])
        move(n, a, a, 4, py)
        move(n, a, a, 6, pc)
        wait_in(b, in_recv.at[n, 2])
        move(n, b, b, 5, px)
        move(n, b, b, 6, pc)

    def plane_rest(n, full, first, many=2):
        for rr, p, i in ((hi, px, 1), (lo, py, 3), (lo, pd, 4), (hi, pd, 5))[first:first + many]:
            ref = full.at[rr, cols(p)]
            wait_in(ref, in_recv.at[n, i])
            move(n, ref, ref, 6, pc)

    def plane_last(n, full):
        wait_in(full.at[:, pl.ds(0, 4 * LANE)], in_recv.at[n, 6])

    plane_first(0, x_in, x_all)

    def wz_one(n, k, p, sl, device, many):
        ref = w2.at[cols(k), cols(p, many * LANE)] if n else w13.at[cols(p, many * LANE), cols(k, 2 * LANE)]
        pair = p if many == 2 else lax.div(p, 2)
        sem = wz_end.at[sl, n] if sl < 3 else wz_mid.at[sl - 3, pair, n]
        return rcopy(ref, ref, wz_send.at[sl, n], sem, (device, t))

    def wz(k, p, sl, device):
        return tuple(wz_one(n, k, p, sl, device, 1) for n in range(2))

    def wz_own(p):
        @pl.when(is_end)
        def _():
            for c in wz(c_end, p, 3, inner):
                c.start()

        @pl.when(is_mid)
        def _():
            for c in wz(c_mid, p, 0, outer) + wz(c_mid, p, 4, inner):
                c.start()

    for c in loc[:3]:
        c.wait()
    wz_own(t)
    for s in (1, 2, 4, 3, 5, 6, 7):
        p = peer(s)
        wait_in(w13.at[cols(p), cols(z, 2 * LANE)], w_recv.at[s, 0])
        wait_in(w2.at[cols(z), cols(p)], w_recv.at[s, 1])
        wz_own(p)

    plane_forward(0, x_all)
    plane_first(1, dy_in, dy_all)

    def each_block(fn):
        lax.fori_loop(0, N_T // 2, lambda p, c: (fn(p), c)[1], 0)

    def pass_weights(n, k, from_sl, to_sl, device):
        def one(p):
            wz_one(n, k, p, from_sl, inner, 2).wait_recv()
            wz_one(n, k, p, to_sl, device, 2).start()
        each_block(one)

    def hop_one():
        pass_weights(0, c_mid2, 4, 1, outer)
        pass_weights(0, c_end, 3, 5, inner)
        pass_weights(1, c_mid2, 4, 1, outer)
        pass_weights(1, c_end, 3, 5, inner)

    def hop_two():
        pass_weights(0, c_end2, 5, 2, outer)

    def hop_three():
        pass_weights(1, c_end2, 5, 2, outer)

    @pl.when(is_mid)
    def _():
        hop_one()

    plane_rest(0, x_all, 0, 4)
    for c in loc[3:5]:
        c.wait()
    wait_in(gain_all.at[:, pl.ds(0, 7 * LANE)], g_recv.at[0])
    plane_last(0, x_all)

    def norm(xf):
        d = xf.shape[1]
        mu = jnp.sum(xf, axis=1, keepdims=True) / d
        sq = jnp.sum(xf * xf, axis=1, keepdims=True) / d
        r = lax.rsqrt(sq - mu * mu + LN_EPS)
        return (xf - mu) * r, r

    def norm_tile(i, carry):
        rr = pl.ds(pl.multiple_of(i * rows, rows), rows)
        xhat, _ = norm(x_all[rr, :].astype(F32))
        h_all[rr, :] = (gain_all[0:1, :] * xhat).astype(BF16)
        return carry

    def block(p):
        return pl.ds(pl.multiple_of(p * rows, rows), rows)

    def piece(p):
        return pl.ds(p * ROWS, ROWS)

    def sum_copy(src, dst, sl, p, device):
        return rcopy(src, dst, sum_send.at[sl], sum_recv.at[sl, p], (device, t))

    def from_end(q, k, p):
        return sum_copy(dw.at[k, piece(p)], outs.at[q, piece(p)], q, p, inner)

    def end_send(q, k, pieces):
        @pl.when(is_end)
        def _():
            for p in pieces:
                from_end(q, k, p).start()

    def uv_tile(i, j):
        return 2 * i + lax.div(j, 4), cols(lax.rem(j, 4), 2 * LANE)

    def forward_chunk(i, k, sl):
        if sl is not None:
            @pl.when(is_end)
            def _():
                wait_in(w13.at[:, cols(k, 2 * LANE)], wz_end.at[sl, 0])

        def tile(j, c):
            rr = block(j)
            uv = dot(h_all[rr, :], w13[:, cols(k, 2 * LANE)])
            at, cc = uv_tile(i, j)
            uv_all[at, :, cc] = uv
            u, v = uv[:, :LANE], uv[:, LANE:]
            act[rr, cols(k)] = (u * jax.nn.sigmoid(u) * v).astype(BF16)
            return c

        lax.fori_loop(0, N_T, tile, 0)

    def turn_act(k):
        def tile(j, c):
            act_t[:, block(j)] = act[block(j), cols(k)].T
            return c
        lax.fori_loop(0, N_T, tile, 0)

    n_cols = dy_all.shape[1] // (2 * LANE)

    def grad_down(k):
        def grad(n, c):
            nn = cols(n, 2 * LANE)
            dw[k, 2 * LANE:, nn] = dot(act_t[...], dy_all[:, nn])
            return c
        lax.fori_loop(0, n_cols, grad, 0)

    def backward_chunk(i, k):
        def tile(j, c):
            rr = block(j)
            da = dot_cols(dy_all[rr, :], w2[cols(k), :])
            at, cc = uv_tile(i, j)
            uv = uv_all[at, :, cc]
            u, v = uv[:, :LANE], uv[:, LANE:]
            sig = jax.nn.sigmoid(u)
            du = (da * v * sig * (1.0 + u * (1.0 - sig))).astype(BF16)
            dv = (da * (u * sig)).astype(BF16)
            duv[rr, cols(2 * k)] = du
            duv[rr, cols(2 * k + 1)] = dv
            duv_t[0:LANE, rr] = du.T
            duv_t[LANE:, rr] = dv.T
            return c

        lax.fori_loop(0, N_T, tile, 0)

        def grad(n, c):
            nn = cols(n, 2 * LANE)
            dw[k, 0:2 * LANE, nn] = dot(duv_t[...], h_all[:, nn])
            return c

        lax.fori_loop(0, n_cols, grad, 0)

    lax.fori_loop(0, N_T, norm_tile, 0)
    x_rows[...] = x_all[block(t), :]

    @pl.when(is_mid)
    def _():
        hop_two()

    forward_chunk(0, c_mid, 0)
    plane_forward(1, dy_all)
    forward_chunk(1, c_end, None)

    @pl.when(is_mid)
    def _():
        hop_three()

    plane_rest(1, dy_all, 0)
    forward_chunk(2, c_mid2, 1)
    turn_act(c_mid2)
    plane_rest(1, dy_all, 2)
    loc[5].wait()
    plane_last(1, dy_all)
    wait_sent(x_all.at[:, pl.ds(0, 7 * LANE)], in_send.at[0])
    grad_down(c_mid2)
    end_send(0, c_mid2, PIECE_ORDER[:2])
    forward_chunk(3, c_end2, 2)

    @pl.when(is_end)
    def _():
        wait_in(w2.at[cols(c_mid2), :], wz_end.at[1, 1])

    backward_chunk(2, c_mid2)
    end_send(0, c_mid2, PIECE_ORDER[2:])

    @pl.when(is_end)
    def _():
        wait_in(w2.at[cols(c_mid), :], wz_end.at[0, 1])
        wait_in(w2.at[cols(c_end2), :], wz_end.at[2, 1])

    def stage0(away, r0, make, base):
        def body(j, c):
            fx, fy = 1 - lax.div(j, 2), 1 - lax.rem(j, 2)
            i = fx + 2 * fy
            away[i] = make(block(pc + fx * flips[1] + fy * flips[2]))
            rcopy(away.at[i], r0.at[i], red_send.at[base // 10], red_recv.at[base + i], (z, pc)).start()
            return c
        lax.fori_loop(0, 4, body, 0)

    def rsend(src, dst, group, sl, device):
        rcopy(src, dst, red_send.at[group], red_recv.at[sl], device).start()

    def rarrived(dst, sl):
        wait_in(dst, red_recv.at[sl])

    a_half, b_half = pl.ds(0, hr), pl.ds(hr, hr)

    def stage1(r0, r1, make, base, between):
        for i in (3, 1, 2, 0):
            rarrived(r0.at[i], base + i)
            r0[i] += make(block((t, px, py, pd)[i]))
            if i == 3:
                rsend(r0.at[3, a_half], r1.at[0], base // 10, base + 4, (z, px))
                rsend(r0.at[3, b_half], r1.at[1], base // 10, base + 5, (z, py))
            if i == 1:
                rsend(r0.at[1, a_half], r1.at[2], base // 10, base + 6, (z, px))
            if i == 2:
                rsend(r0.at[2, b_half], r1.at[3], base // 10, base + 7, (z, py))
            for p in between.get(i, ()):
                pass_in(0, c_mid2, p)

    def stage2(r0, r1, r2, base):
        rarrived(r1.at[0], base + 4)
        r0[2, 0:hr] += r1[0]
        rsend(r0.at[2, a_half], r2.at[0], base // 10, base + 8, (z, py))
        rarrived(r1.at[1], base + 5)
        r0[1, hr:rows] += r1[1]
        rsend(r0.at[1, b_half], r2.at[1], base // 10, base + 9, (z, px))

    def stage3(r0, r1, base):
        rarrived(r1.at[2], base + 6)
        r0[0, 0:hr] += r1[2]
        rarrived(r1.at[3], base + 7)
        r0[0, hr:rows] += r1[3]

    def stage4(r0, r2, base):
        rarrived(r2.at[0], base + 8)
        r0[0, 0:hr] += r2[0]
        rarrived(r2.at[1], base + 9)
        r0[0, hr:rows] += r2[1]

    def make_m(rr):
        return dot(act[rr, :], w2[...])

    def make_dh(rr):
        return dot_cols(duv[rr, :], w13[...])

    def finish(src, p):
        for s in (6, 7, 2, 4, 3, 5, 1):
            q = peer(s)
            rcopy(src.at[:, cols(q)], dw_out.at[t, piece(p)], fin_sem.at[0], fin_sem.at[1], (z, q)).start()
        pltpu.make_async_copy(src.at[:, cols(t)], dw_out.at[t, piece(p)], fin_sem.at[2]).start()

    def pass_in(q, k, p):
        @pl.when(is_mid)
        def _():
            ref = outs.at[q, piece(p)]
            sum_copy(ref, ref, q, p, outer).wait_recv()
            outs[q, p * ROWS:(p + 1) * ROWS] += dw[k, p * ROWS:(p + 1) * ROWS]
            sum_copy(ref, ins.at[q, piece(p)], 3 + q, p, inner).start()

    def pass_out(p):
        @pl.when(is_mid)
        def _():
            ref = ins.at[1, piece(p)]
            sum_copy(ref, ref, 4, p, inner).wait_recv()
            ins[1, p * ROWS:(p + 1) * ROWS] += dw[c_end, p * ROWS:(p + 1) * ROWS]
            sum_copy(ref, ref, 5, p, outer).start()

    def last_mid(p):
        @pl.when(is_mid)
        def _():
            a, b = outs.at[2, piece(p)], ins.at[0, piece(p)]
            sum_copy(b, b, 3, p, inner).wait_recv()
            sum_copy(a, a, 2, p, outer).wait_recv()
            rr = slice(p * ROWS, (p + 1) * ROWS)
            outs[2, rr] += ins[0, rr] + dw[c_mid, rr]
            finish(a, p)

    def last_end(p):
        @pl.when(is_end)
        def _():
            a = ins.at[1, piece(p)]
            sum_copy(a, a, 5, p, inner).wait_recv()
            rr = slice(p * ROWS, (p + 1) * ROWS)
            ins[1, rr] += dw[c_end, rr]
            finish(a, p)

    stage0(m_away, m0, make_m, 0)
    stage1(m0, m1, make_m, 0, {3: PIECE_ORDER[:1], 2: PIECE_ORDER[1:2]})
    turn_act(c_end2)
    grad_down(c_end2)
    pass_in(0, c_mid2, PIECE_ORDER[2])
    backward_chunk(3, c_end2)
    end_send(1, c_end2, PIECE_ORDER)
    turn_act(c_mid)
    grad_down(c_mid)
    pass_in(0, c_mid2, PIECE_ORDER[3])
    backward_chunk(0, c_mid)
    end_send(2, c_mid, PIECE_ORDER)
    stage2(m0, m1, m2, 0)
    pass_in(0, c_mid2, PIECE_ORDER[4])
    turn_act(c_end)
    grad_down(c_end)
    backward_chunk(1, c_end)
    pass_in(0, c_mid2, PIECE_ORDER[5])
    stage0(e_away, e0, make_dh, 10)
    stage1(e0, e1, make_dh, 10, {})

    def spread(src, dst, group, local):
        for s in (6, 7, 2, 4, 3, 5, 1):
            q = peer(s)
            rsend(src.at[:, cols(q)], dst.at[block(t), :], group, group + 18, (z, q))
        c = pltpu.make_async_copy(src.at[:, cols(t)], dst.at[block(t), :], local_sem.at[local])
        c.start()
        loc.append(c)

    def make_y():
        stage4(m0, m2, 0)
        y_rows[...] = (x_rows[...].astype(F32) + m0[0]).astype(BF16)
        spread(y_rows, y_out, 2, 6)

    def make_dx():
        stage4(e0, e2, 10)
        xhat, r = norm(x_rows[...].astype(F32))
        d = xhat.shape[1]
        dh = e0[0]
        e = dh * gain_all[0:1, :]
        e_mean = jnp.sum(e, axis=1, keepdims=True) / d
        ex_mean = jnp.sum(e * xhat, axis=1, keepdims=True) / d
        dy_rows = dy_all[block(t), :].astype(F32)
        dx_rows[...] = (dy_rows + r * (e - e_mean - xhat * ex_mean)).astype(BF16)
        dg_rows[...] = jnp.sum((dh * xhat).reshape(rows // 8, 8, d), axis=0)
        for s in order:
            rsend(dg_rows.at[:, cols(peer(s))], dg_plane.at[s - 1], 4, 22, (z, peer(s)))
        spread(dx_rows, dx_out, 3, 7)

    def gain_plane():
        total = dg_rows[:, cols(t)]
        rarrived(dg_plane, 22)
        for s in range(1, 8):
            total = total + dg_plane[s - 1]
        dg_line[0] = total
        for s in range(1, 4):
            rsend(dg_line.at[0], dg_line.at[s], 5, 23, (lax.rem(z + s, 4), t))

    def gain_line():
        rarrived(dg_line.at[pl.ds(1, 3)], 23)
        parts = [dg_line[lax.rem(z - s + 4, 4)] for s in range(4)]
        dg_out[...] = (parts[0] + parts[1]) + (parts[2] + parts[3])

    per = 33.7 / PIECES
    plan = [(84, lambda: stage3(m0, m1, 0)), (108.6, make_y),
            (108.5, lambda: stage2(e0, e1, e2, 10)), (121, lambda: stage3(e0, e1, 10)),
            (131, make_dx), (149.5, gain_plane), (157, gain_line)]
    for n, p in enumerate(PIECE_ORDER):
        done = 86 + per * (n + 1)
        plan.append((done, lambda p=p: pass_in(1, c_end2, p)))
        plan.append((done + per + 1, lambda p=p: pass_out(p)))
        plan.append((done + 2 * per + 2, lambda p=p: last_end(p)))
        plan.append((done + 33.7, lambda p=p: last_mid(p)))
    for _, fn in sorted(plan, key=lambda e: e[0]):
        fn()

    seven = pl.ds(0, 7 * LANE)
    rarrived(y_out.at[pl.ds(0, 7 * rows), :], 20)
    rarrived(dx_out.at[pl.ds(0, 7 * rows), :], 21)
    wait_in(dw_out.at[pl.ds(0, 7)], fin_sem.at[1])
    pltpu.make_async_copy(dw_out.at[0], dw_out.at[0], fin_sem.at[2]).wait()
    for c in loc[6:]:
        c.wait()
    wait_sent(dw_out.at[pl.ds(0, 7)], fin_sem.at[0])
    for n in range(3):
        wait_sent(w13.at[pl.ds(0, LANE), seven], w_send.at[n])
    wait_sent(gain_all.at[:, seven], w_send.at[3])
    wait_sent(dy_all.at[:, seven], in_send.at[1])
    for n, ref in enumerate((uv_all.at[pl.ds(0, 7)], uv_all.at[pl.ds(0, 7)], y_rows.at[:, seven], dx_rows.at[:, seven],
                             dg_rows.at[:, seven], dg_line.at[pl.ds(1, 3)])):
        wait_sent(ref, red_send.at[n])

    def chunk_sent(sl):
        wait_sent(w13.at[:, cols(0, 2 * LANE)], wz_send.at[sl, 0])
        wait_sent(w2.at[cols(0), :], wz_send.at[sl, 1])

    @pl.when(is_end)
    def _():
        chunk_sent(3)
        for q in range(3):
            wait_sent(dw.at[0], sum_send.at[q])

    @pl.when(is_mid)
    def _():
        for sl in (0, 1, 2, 4, 5):
            chunk_sent(sl)
        for q in (3, 4, 5):
            wait_sent(dw.at[0], sum_send.at[q])


def place_kernel(y_in, dx_in, dw_in, dg_in, y_out, dx_out, dw1_out, dw3_out, dw2_out, dg_out):
    y_out[...] = y_in[...]
    dx_out[...] = dx_in[...]
    for s in range(N_T):
        at = slice(s * LANE, (s + 1) * LANE)
        dw1_out[:, at] = dw_in[s, 0:LANE].T
        dw3_out[:, at] = dw_in[s, LANE:2 * LANE].T
        dw2_out[at, :] = dw_in[s, 2 * LANE:]
    dg_out[...] = jnp.sum(dg_in[...], axis=0, keepdims=True)


def solution(mesh):
    def local_step(x_blk, dy_blk, gain_blk, w1_blk, w3_blk, w2_blk):
        tokens, lane = x_blk.shape
        d = lane * N_T
        f = w1_blk.shape[1] // N_T * N_Z
        rows = tokens // N_T
        any_spec = pl.BlockSpec(memory_space=pl.ANY)
        vmem = pl.BlockSpec(memory_space=pltpu.VMEM)
        s = jax.ShapeDtypeStruct
        V = pltpu.VMEM
        dma = pltpu.SemaphoreType.DMA
        red = [V((4, rows, d), F32), V((4, rows, d), F32), V((4, rows // 2, d), F32), V((2, rows // 2, d), F32)]
        y, dx, dw, dg = pl.pallas_call(
            step_kernel,
            out_shape=(s((tokens, lane), BF16), s((tokens, lane), BF16), s((N_T, 384, lane), F32), s((8, lane), F32)),
            in_specs=[any_spec] * 6,
            out_specs=[any_spec] * 3 + [vmem],
            scratch_shapes=[
                V((tokens, d), BF16), V((tokens, d), BF16), V((tokens, d), BF16), V((1, d), F32),
                V((d, 2 * f), BF16), V((f, d), BF16), V((tokens, f), BF16), V((lane, tokens), BF16),
                V((2 * lane, tokens), BF16), V((N_Z, 384, d), F32), V((N_T, rows, d), F32)] + red + red[1:] + [
                V((3, 384, d), F32), V((2, 384, d), F32),
                V((rows, d), BF16), V((rows, d), BF16), V((rows, d), BF16), V((8, d), F32),
                V((7, 8, lane), F32), V((4, 8, lane), F32),
                dma((4,)), dma((N_T, 2)), dma((1,)), dma((2,)), dma((2, 7)), dma((6, 2)), dma((3, 2)),
                dma((3, N_T // 2, 2)), dma((6,)), dma((6, PIECES)), dma((3,)), dma((6,)), dma((24,)), dma((8,))],
            compiler_params=pltpu.CompilerParams(collective_id=0, has_side_effects=True, vmem_limit_bytes=67043328),
            name="step",
        )(x_blk, dy_blk, gain_blk[None, :], w1_blk, w3_blk, w2_blk)
        f_z = w1_blk.shape[1]
        y, dx, dw1, dw3, dw2, dg = pl.pallas_call(
            place_kernel,
            out_shape=(s((tokens, lane), BF16), s((tokens, lane), BF16), s((lane, f_z), F32), s((lane, f_z), F32),
                       s((f_z, lane), F32), s((1, lane), F32)),
            in_specs=[vmem] * 4, out_specs=[vmem] * 6, name="place",
        )(y, dx, dw, dg)
        return y, dx, dw1, dw3, dw2, dg[0]

    return jax.shard_map(
        local_step, mesh=mesh,
        in_specs=(P("ty", "tx"), P("ty", "tx"), P("tx"), P("tx", "ty"), P("tx", "ty"), P("ty", "tx")),
        out_specs=(P("ty", "tx"), P("ty", "tx"), P("tx", "ty"), P("tx", "ty"), P("ty", "tx"), P("tx")),
        check_vma=False)
```

```python
import jax
import jax.numpy as jnp
from jax import lax
from jax.experimental import pallas as pl
from jax.experimental.pallas import tpu as pltpu
from jax.sharding import PartitionSpec as P

LN_EPS = 1e-6
F32 = jnp.float32
BF16 = jnp.bfloat16
MESH = pl.DeviceIdType.MESH
LANE = 128
WIDE = LANE + LANE
ORDER = (2, 4, 3, 5, 6, 7, 1)
N_T = 8
N_Z = 4
PIECES = 6
CHUNK = 3 * LANE
ROWS = CHUNK // PIECES
PIECE_ORDER = (4, 5, 0, 1, 2, 3)


def cols(k, width=LANE):
    return pl.ds(pl.multiple_of(k * width, width), width)


def dot(a, b):
    return jnp.dot(a, b, preferred_element_type=F32)


def dot_cols(a, b):
    return lax.dot_general(a, b, (((1,), (1,)), ((), ())), preferred_element_type=F32)


def step_kernel(x_in, dy_in, g_in, w1_in, w3_in, w2_in,
                y_out, dx_out, dw_out, dg_out,
                x_all, h_all, dy_all, gain_all, w13, w2, act, act_t, duv_t, dw, uv_all,
                m_away, m0, m1, m2, e0, e1, e2, outs, ins,
                x_rows, y_rows, dx_rows, dg_rows, dg_plane, dg_line,
                w_send, w_recv, g_recv, in_send, in_recv, wz_send, wz_end, wz_mid, sum_send, sum_recv,
                fin_sem, red_send, red_recv, local_sem):
    z = lax.axis_index("ty")
    t = lax.axis_index("tx")
    core = lax.rem(t, 2)
    xbit = lax.rem(lax.div(t, 2), 2)
    ybit = lax.div(t, 4)
    flips = [size - 2 * size * bit for size, bit in ((1, core), (2, xbit), (4, ybit))]
    duv = x_all
    e_away = uv_all.at[pl.ds(4, 4)]

    def peer(s):
        out = t
        for bit in range(3):
            if s >> bit & 1:
                out = out + flips[bit]
        return out

    px, py, pd, pc = peer(2), peer(4), peer(6), peer(1)
    tokens = x_all.shape[0]
    half = tokens // 2
    rows = tokens // N_T
    hr = rows // 2

    low = lax.div(3 - z, 2)
    is_end = jnp.logical_or(z == 0, z == 3)
    is_mid = jnp.logical_or(z == 1, z == 2)
    c_end = 3 - 3 * low
    c_mid = 2 - low
    c_mid2 = 3 - c_mid
    c_end2 = 3 - c_end
    inner = z + 2 * low - 1
    outer = z - 2 * low + 1

    def rcopy(src, dst, ssem, rsem, device):
        return pltpu.make_async_remote_copy(src_ref=src, dst_ref=dst, send_sem=ssem, recv_sem=rsem,
                                            device_id=device, device_id_type=MESH)

    def wait_sent(ref, sem):
        rcopy(ref, ref, sem, sem, (z, pc)).wait_send()

    def wait_in(ref, sem):
        rcopy(ref, ref, sem, sem, (z, pc)).wait_recv()

    loc = [
        pltpu.make_async_copy(w1_in.at[:, cols(t)], w13.at[cols(t), cols(2 * z)], local_sem.at[0]),
        pltpu.make_async_copy(w3_in.at[:, cols(t)], w13.at[cols(t), cols(2 * z + 1)], local_sem.at[1]),
        pltpu.make_async_copy(w2_in.at[cols(t), :], w2.at[cols(z), cols(t)], local_sem.at[2]),
        pltpu.make_async_copy(g_in, gain_all.at[:, cols(t)], local_sem.at[3]),
        pltpu.make_async_copy(x_in, x_all.at[:, cols(t)], local_sem.at[4]),
        pltpu.make_async_copy(dy_in, dy_all.at[:, cols(t)], local_sem.at[5]),
    ]
    for c in loc:
        c.start()
    barrier = pltpu.get_barrier_semaphore()
    for s in ORDER:
        pl.semaphore_signal(barrier, inc=1, device_id=(z, peer(s)), device_id_type=MESH)
    for s in range(1, N_Z):
        pl.semaphore_signal(barrier, inc=1, device_id=(lax.rem(z + s, N_Z), t), device_id_type=MESH)
    pl.semaphore_wait(barrier, N_T - 1 + N_Z - 1)

    for s in ORDER:
        p = peer(s)
        rcopy(w1_in.at[:, cols(p)], w13.at[cols(t), cols(2 * z)], w_send.at[0], w_recv.at[s, 0], (z, p)).start()
        rcopy(w3_in.at[:, cols(p)], w13.at[cols(t), cols(2 * z + 1)], w_send.at[1], w_recv.at[s, 0], (z, p)).start()
        rcopy(w2_in.at[cols(p), :], w2.at[cols(z), cols(t)], w_send.at[2], w_recv.at[s, 1], (z, p)).start()
        rcopy(g_in, gain_all.at[:, cols(t)], w_send.at[3], g_recv.at[0], (z, p)).start()

    lo, hi = pl.ds(0, half), pl.ds(half, half)

    def move(n, src, dst, i, device):
        rcopy(src, dst, in_send.at[n], in_recv.at[n, i], (z, device)).start()

    def plane_first(n, src, full):
        move(n, src.at[lo], full.at[lo, cols(t)], 0, px)
        move(n, src.at[hi], full.at[hi, cols(t)], 2, py)
        move(n, src.at[hi], full.at[hi, cols(t)], 1, px)
        move(n, src.at[lo], full.at[lo, cols(t)], 3, py)
        move(n, src, full.at[:, cols(t)], 6, pc)

    def plane_forward(n, full):
        a, b = full.at[lo, cols(px)], full.at[hi, cols(py)]
        wait_in(a, in_recv.at[n, 0])
        move(n, a, a, 4, py)
        move(n, a, a, 6, pc)
        wait_in(b, in_recv.at[n, 2])
        move(n, b, b, 5, px)
        move(n, b, b, 6, pc)

    def plane_rest(n, full, first, many=2):
        for rr, p, i in ((hi, px, 1), (lo, py, 3), (lo, pd, 4), (hi, pd, 5))[first:first + many]:
            ref = full.at[rr, cols(p)]
            wait_in(ref, in_recv.at[n, i])
            move(n, ref, ref, 6, pc)

    def plane_last(n, full):
        wait_in(full.at[:, pl.ds(0, 4 * LANE)], in_recv.at[n, 6])

    plane_first(0, x_in, x_all)

    def wz_one(n, k, p, sl, device, many):
        ref = w2.at[cols(k), cols(p, many * LANE)] if n else w13.at[cols(p, many * LANE), cols(k, WIDE)]
        pair = p if many == 2 else lax.div(p, 2)
        sem = wz_end.at[sl, n] if sl < 3 else wz_mid.at[sl - 3, pair, n]
        return rcopy(ref, ref, wz_send.at[sl, n], sem, (device, t))

    def wz(k, p, sl, device):
        return tuple(wz_one(n, k, p, sl, device, 1) for n in range(2))

    def wz_own(p):
        @pl.when(is_end)
        def _():
            for c in wz(c_end, p, 3, inner):
                c.start()

        @pl.when(is_mid)
        def _():
            for c in wz(c_mid, p, 0, outer) + wz(c_mid, p, 4, inner):
                c.start()

    for c in loc[:3]:
        c.wait()
    wz_own(t)
    for s in ORDER[-1:] + ORDER[:-1]:
        p = peer(s)
        wait_in(w13.at[cols(p), cols(z, WIDE)], w_recv.at[s, 0])
        wait_in(w2.at[cols(z), cols(p)], w_recv.at[s, 1])
        wz_own(p)

    plane_forward(0, x_all)
    plane_first(1, dy_in, dy_all)

    def each_block(fn):
        lax.fori_loop(0, N_T // 2, lambda p, c: (fn(p), c)[1], 0)

    def pass_weights(n, k, from_sl, to_sl, device):
        def one(p):
            wz_one(n, k, p, from_sl, inner, 2).wait_recv()
            wz_one(n, k, p, to_sl, device, 2).start()
        each_block(one)

    def hop_one():
        pass_weights(0, c_mid2, 4, 1, outer)
        pass_weights(0, c_end, 3, 5, inner)
        pass_weights(1, c_mid2, 4, 1, outer)
        pass_weights(1, c_end, 3, 5, inner)

    def hop_two():
        pass_weights(0, c_end2, 5, 2, outer)

    def hop_three():
        pass_weights(1, c_end2, 5, 2, outer)

    @pl.when(is_mid)
    def _():
        hop_one()

    plane_rest(0, x_all, 0, 4)
    for c in loc[3:5]:
        c.wait()
    wait_in(gain_all.at[:, pl.ds(0, 7 * LANE)], g_recv.at[0])
    plane_last(0, x_all)

    def norm(xf):
        d = xf.shape[1]
        mu = jnp.sum(xf, axis=1, keepdims=True) / d
        sq = jnp.sum(xf * xf, axis=1, keepdims=True) / d
        r = lax.rsqrt(sq - mu * mu + LN_EPS)
        return (xf - mu) * r, r

    def norm_tile(i, carry):
        rr = pl.ds(pl.multiple_of(i * rows, rows), rows)
        xhat, _ = norm(x_all[rr, :].astype(F32))
        h_all[rr, :] = (gain_all[0:1, :] * xhat).astype(BF16)
        return carry

    def block(p):
        return pl.ds(pl.multiple_of(p * rows, rows), rows)

    def piece(p):
        return pl.ds(p * ROWS, ROWS)

    def sum_copy(src, dst, sl, p, device):
        return rcopy(src, dst, sum_send.at[sl], sum_recv.at[sl, p], (device, t))

    def from_end(q, k, p):
        return sum_copy(dw.at[k, piece(p)], outs.at[q, piece(p)], q, p, inner)

    def end_send(q, k, pieces):
        @pl.when(is_end)
        def _():
            for p in pieces:
                from_end(q, k, p).start()

    def uv_tile(i, j):
        return 2 * i + lax.div(j, 4), cols(lax.rem(j, 4), WIDE)

    def forward_chunk(i, k, sl):
        if sl is not None:
            @pl.when(is_end)
            def _():
                wait_in(w13.at[:, cols(k, WIDE)], wz_end.at[sl, 0])

        def tile(j, c):
            rr = block(j)
            uv = dot(h_all[rr, :], w13[:, cols(k, WIDE)])
            at, cc = uv_tile(i, j)
            uv_all[at, :, cc] = uv
            u, v = uv[:, :LANE], uv[:, LANE:]
            act[rr, cols(k)] = (u * jax.nn.sigmoid(u) * v).astype(BF16)
            return c

        lax.fori_loop(0, N_T, tile, 0)

    def turn_act(k):
        def tile(j, c):
            act_t[:, block(j)] = act[block(j), cols(k)].T
            return c
        lax.fori_loop(0, N_T, tile, 0)

    n_cols = dy_all.shape[1] // (WIDE)

    def grad_down(k):
        def grad(n, c):
            nn = cols(n, WIDE)
            dw[k, WIDE:, nn] = dot(act_t[...], dy_all[:, nn])
            return c
        lax.fori_loop(0, n_cols, grad, 0)

    def backward_chunk(i, k):
        def tile(j, c):
            rr = block(j)
            da = dot_cols(dy_all[rr, :], w2[cols(k), :])
            at, cc = uv_tile(i, j)
            uv = uv_all[at, :, cc]
            u, v = uv[:, :LANE], uv[:, LANE:]
            sig = jax.nn.sigmoid(u)
            du = (da * v * sig * (1.0 + u * (1.0 - sig))).astype(BF16)
            dv = (da * (u * sig)).astype(BF16)
            duv[rr, cols(2 * k)] = du
            duv[rr, cols(2 * k + 1)] = dv
            duv_t[0:LANE, rr] = du.T
            duv_t[LANE:, rr] = dv.T
            return c

        lax.fori_loop(0, N_T, tile, 0)

        def grad(n, c):
            nn = cols(n, WIDE)
            dw[k, 0:WIDE, nn] = dot(duv_t[...], h_all[:, nn])
            return c

        lax.fori_loop(0, n_cols, grad, 0)

    lax.fori_loop(0, N_T, norm_tile, 0)
    x_rows[...] = x_all[block(t), :]

    @pl.when(is_mid)
    def _():
        hop_two()

    forward_chunk(0, c_mid, 0)
    plane_forward(1, dy_all)
    forward_chunk(1, c_end, None)

    @pl.when(is_mid)
    def _():
        hop_three()

    plane_rest(1, dy_all, 0)
    forward_chunk(2, c_mid2, 1)
    turn_act(c_mid2)
    plane_rest(1, dy_all, 2)
    loc[5].wait()
    plane_last(1, dy_all)
    wait_sent(x_all.at[:, pl.ds(0, 7 * LANE)], in_send.at[0])
    grad_down(c_mid2)
    end_send(0, c_mid2, PIECE_ORDER[:2])
    forward_chunk(3, c_end2, 2)

    @pl.when(is_end)
    def _():
        wait_in(w2.at[cols(c_mid2), :], wz_end.at[1, 1])

    backward_chunk(2, c_mid2)
    end_send(0, c_mid2, PIECE_ORDER[2:])

    @pl.when(is_end)
    def _():
        wait_in(w2.at[cols(c_mid), :], wz_end.at[0, 1])
        wait_in(w2.at[cols(c_end2), :], wz_end.at[2, 1])

    def stage0(away, r0, make, base):
        def body(j, c):
            fx, fy = 1 - lax.div(j, 2), 1 - lax.rem(j, 2)
            i = fx + 2 * fy
            away[i] = make(block(pc + fx * flips[1] + fy * flips[2]))
            rcopy(away.at[i], r0.at[i], red_send.at[base // 10], red_recv.at[base + i], (z, pc)).start()
            return c
        lax.fori_loop(0, 4, body, 0)

    def rsend(src, dst, group, sl, device):
        rcopy(src, dst, red_send.at[group], red_recv.at[sl], device).start()

    def rarrived(dst, sl):
        wait_in(dst, red_recv.at[sl])

    a_half, b_half = pl.ds(0, hr), pl.ds(hr, hr)

    def stage1(r0, r1, make, base, between):
        for i in (3, 1, 2, 0):
            rarrived(r0.at[i], base + i)
            r0[i] += make(block((t, px, py, pd)[i]))
            if i == 3:
                rsend(r0.at[3, a_half], r1.at[0], base // 10, base + 4, (z, px))
                rsend(r0.at[3, b_half], r1.at[1], base // 10, base + 5, (z, py))
            if i == 1:
                rsend(r0.at[1, a_half], r1.at[2], base // 10, base + 6, (z, px))
            if i == 2:
                rsend(r0.at[2, b_half], r1.at[3], base // 10, base + 7, (z, py))
            for p in between.get(i, ()):
                pass_in(0, c_mid2, p)

    def stage2(r0, r1, r2, base):
        rarrived(r1.at[0], base + 4)
        r0[2, 0:hr] += r1[0]
        rsend(r0.at[2, a_half], r2.at[0], base // 10, base + 8, (z, py))
        rarrived(r1.at[1], base + 5)
        r0[1, hr:rows] += r1[1]
        rsend(r0.at[1, b_half], r2.at[1], base // 10, base + 9, (z, px))

    def stage3(r0, r1, base):
        rarrived(r1.at[2], base + 6)
        r0[0, 0:hr] += r1[2]
        rarrived(r1.at[3], base + 7)
        r0[0, hr:rows] += r1[3]

    def stage4(r0, r2, base):
        rarrived(r2.at[0], base + 8)
        r0[0, 0:hr] += r2[0]
        rarrived(r2.at[1], base + 9)
        r0[0, hr:rows] += r2[1]

    def make_m(rr):
        return dot(act[rr, :], w2[...])

    def make_dh(rr):
        return dot_cols(duv[rr, :], w13[...])

    def finish(src, p):
        for s in ORDER:
            q = peer(s)
            rcopy(src.at[:, cols(q)], dw_out.at[t, piece(p)], fin_sem.at[0], fin_sem.at[1], (z, q)).start()
        pltpu.make_async_copy(src.at[:, cols(t)], dw_out.at[t, piece(p)], fin_sem.at[2]).start()

    def pass_in(q, k, p):
        @pl.when(is_mid)
        def _():
            ref = outs.at[q, piece(p)]
            sum_copy(ref, ref, q, p, outer).wait_recv()
            outs[q, piece(p)] += dw[k, piece(p)]
            sum_copy(ref, ins.at[q, piece(p)], 3 + q, p, inner).start()

    def pass_out(p):
        @pl.when(is_mid)
        def _():
            ref = ins.at[1, piece(p)]
            sum_copy(ref, ref, 4, p, inner).wait_recv()
            ins[1, piece(p)] += dw[c_end, piece(p)]
            sum_copy(ref, ref, 5, p, outer).start()

    def last_mid(p):
        @pl.when(is_mid)
        def _():
            a, b = outs.at[2, piece(p)], ins.at[0, piece(p)]
            sum_copy(b, b, 3, p, inner).wait_recv()
            sum_copy(a, a, 2, p, outer).wait_recv()
            rr = piece(p)
            outs[2, rr] += ins[0, rr] + dw[c_mid, rr]
            finish(a, p)

    def last_end(p):
        @pl.when(is_end)
        def _():
            a = ins.at[1, piece(p)]
            sum_copy(a, a, 5, p, inner).wait_recv()
            rr = piece(p)
            ins[1, rr] += dw[c_end, rr]
            finish(a, p)

    stage0(m_away, m0, make_m, 0)
    stage1(m0, m1, make_m, 0, {3: PIECE_ORDER[:1], 2: PIECE_ORDER[1:2]})
    turn_act(c_end2)
    grad_down(c_end2)
    pass_in(0, c_mid2, PIECE_ORDER[2])
    backward_chunk(3, c_end2)
    end_send(1, c_end2, PIECE_ORDER)
    turn_act(c_mid)
    grad_down(c_mid)
    pass_in(0, c_mid2, PIECE_ORDER[3])
    backward_chunk(0, c_mid)
    end_send(2, c_mid, PIECE_ORDER)
    stage2(m0, m1, m2, 0)
    pass_in(0, c_mid2, PIECE_ORDER[4])
    turn_act(c_end)
    grad_down(c_end)
    backward_chunk(1, c_end)
    pass_in(0, c_mid2, PIECE_ORDER[5])
    stage0(e_away, e0, make_dh, 10)
    stage1(e0, e1, make_dh, 10, {})

    def spread(src, dst, group, local):
        for s in ORDER:
            q = peer(s)
            rsend(src.at[:, cols(q)], dst.at[block(t), :], group, group + 18, (z, q))
        c = pltpu.make_async_copy(src.at[:, cols(t)], dst.at[block(t), :], local_sem.at[local])
        c.start()
        loc.append(c)

    def make_y():
        stage4(m0, m2, 0)
        y_rows[...] = (x_rows[...].astype(F32) + m0[0]).astype(BF16)
        spread(y_rows, y_out, 2, 6)

    def make_dx():
        stage4(e0, e2, 10)
        xhat, r = norm(x_rows[...].astype(F32))
        d = xhat.shape[1]
        dh = e0[0]
        e = dh * gain_all[0:1, :]
        e_mean = jnp.sum(e, axis=1, keepdims=True) / d
        ex_mean = jnp.sum(e * xhat, axis=1, keepdims=True) / d
        dy_rows = dy_all[block(t), :].astype(F32)
        dx_rows[...] = (dy_rows + r * (e - e_mean - xhat * ex_mean)).astype(BF16)
        dg_rows[...] = jnp.sum((dh * xhat).reshape(rows // 8, 8, d), axis=0)
        for s in ORDER:
            rsend(dg_rows.at[:, cols(peer(s))], dg_plane.at[s - 1], 4, 22, (z, peer(s)))
        spread(dx_rows, dx_out, 3, 7)

    def gain_plane():
        total = dg_rows[:, cols(t)]
        rarrived(dg_plane, 22)
        for s in range(1, 8):
            total = total + dg_plane[s - 1]
        dg_line[0] = total
        for s in range(1, 4):
            rsend(dg_line.at[0], dg_line.at[s], 5, 23, (lax.rem(z + s, 4), t))

    def gain_line():
        rarrived(dg_line.at[pl.ds(1, 3)], 23)
        parts = [dg_line[lax.rem(z - s + 4, 4)] for s in range(4)]
        dg_out[...] = sum(parts[1:], parts[0])

    per = 33.7 / PIECES
    plan = [(84, lambda: stage3(m0, m1, 0)), (108.6, make_y),
            (108.5, lambda: stage2(e0, e1, e2, 10)), (121, lambda: stage3(e0, e1, 10)),
            (131, make_dx), (149.5, gain_plane), (157, gain_line)]
    for n, p in enumerate(PIECE_ORDER):
        done = 86 + per * (n + 1)
        plan.append((done, lambda p=p: pass_in(1, c_end2, p)))
        plan.append((done + per + 1, lambda p=p: pass_out(p)))
        plan.append((done + 2 * per + 2, lambda p=p: last_end(p)))
        plan.append((done + 33.7, lambda p=p: last_mid(p)))
    for _, fn in sorted(plan, key=lambda e: e[0]):
        fn()

    seven = pl.ds(0, 7 * LANE)
    rarrived(y_out.at[pl.ds(0, 7 * rows), :], 20)
    rarrived(dx_out.at[pl.ds(0, 7 * rows), :], 21)
    wait_in(dw_out.at[pl.ds(0, 7)], fin_sem.at[1])
    pltpu.make_async_copy(dw_out.at[0], dw_out.at[0], fin_sem.at[2]).wait()
    for c in loc[6:]:
        c.wait()
    wait_sent(dw_out.at[pl.ds(0, 7)], fin_sem.at[0])
    for n in range(3):
        wait_sent(w13.at[pl.ds(0, LANE), seven], w_send.at[n])
    wait_sent(gain_all.at[:, seven], w_send.at[3])
    wait_sent(dy_all.at[:, seven], in_send.at[1])
    for n, ref in enumerate((uv_all.at[pl.ds(0, 7)], uv_all.at[pl.ds(0, 7)], y_rows.at[:, seven], dx_rows.at[:, seven],
                             dg_rows.at[:, seven], dg_line.at[pl.ds(1, 3)])):
        wait_sent(ref, red_send.at[n])

    def chunk_sent(sl):
        wait_sent(w13.at[:, cols(0, WIDE)], wz_send.at[sl, 0])
        wait_sent(w2.at[cols(0), :], wz_send.at[sl, 1])

    @pl.when(is_end)
    def _():
        chunk_sent(3)
        for q in range(3):
            wait_sent(dw.at[0], sum_send.at[q])

    @pl.when(is_mid)
    def _():
        for sl in range(6):
            if sl != 3:
                chunk_sent(sl)
        for q in range(3, 6):
            wait_sent(dw.at[0], sum_send.at[q])


def place_kernel(y_in, dx_in, dw_in, dg_in, y_out, dx_out, dw1_out, dw3_out, dw2_out, dg_out):
    y_out[...] = y_in[...]
    dx_out[...] = dx_in[...]
    for s in range(N_T):
        at = slice(s * LANE, (s + 1) * LANE)
        dw1_out[:, at] = dw_in[s, 0:LANE].T
        dw3_out[:, at] = dw_in[s, LANE:WIDE].T
        dw2_out[at, :] = dw_in[s, WIDE:]
    dg_out[...] = jnp.sum(dg_in[...], axis=0, keepdims=True)


def solution(mesh):
    def local_step(x_blk, dy_blk, gain_blk, w1_blk, w3_blk, w2_blk):
        tokens, lane = x_blk.shape
        d = lane * N_T
        f = w1_blk.shape[1] // N_T * N_Z
        rows = tokens // N_T
        any_spec = pl.BlockSpec(memory_space=pl.ANY)
        vmem = pl.BlockSpec(memory_space=pltpu.VMEM)
        s = jax.ShapeDtypeStruct
        V = pltpu.VMEM
        dma = pltpu.SemaphoreType.DMA
        red = [V((4, rows, d), F32), V((4, rows, d), F32), V((4, rows // 2, d), F32), V((2, rows // 2, d), F32)]
        y, dx, dw, dg = pl.pallas_call(
            step_kernel,
            out_shape=(s((tokens, lane), BF16), s((tokens, lane), BF16), s((N_T, CHUNK, lane), F32), s((8, lane), F32)),
            in_specs=[any_spec] * 6,
            out_specs=[any_spec] * 3 + [vmem],
            scratch_shapes=[
                V((tokens, d), BF16), V((tokens, d), BF16), V((tokens, d), BF16), V((1, d), F32),
                V((d, 2 * f), BF16), V((f, d), BF16), V((tokens, f), BF16), V((lane, tokens), BF16),
                V((WIDE, tokens), BF16), V((N_Z, CHUNK, d), F32), V((N_T, rows, d), F32)] + red + red[1:] + [
                V((3, CHUNK, d), F32), V((2, CHUNK, d), F32),
                V((rows, d), BF16), V((rows, d), BF16), V((rows, d), BF16), V((8, d), F32),
                V((7, 8, lane), F32), V((4, 8, lane), F32),
                dma((4,)), dma((N_T, 2)), dma((1,)), dma((2,)), dma((2, 7)), dma((6, 2)), dma((3, 2)),
                dma((3, N_T // 2, 2)), dma((6,)), dma((6, PIECES)), dma((3,)), dma((6,)), dma((24,)), dma((8,))],
            compiler_params=pltpu.CompilerParams(collective_id=0, has_side_effects=True, vmem_limit_bytes=67043328),
            name="step",
        )(x_blk, dy_blk, gain_blk[None, :], w1_blk, w3_blk, w2_blk)
        f_z = w1_blk.shape[1]
        y, dx, dw1, dw3, dw2, dg = pl.pallas_call(
            place_kernel,
            out_shape=(s((tokens, lane), BF16), s((tokens, lane), BF16), s((lane, f_z), F32), s((lane, f_z), F32),
                       s((f_z, lane), F32), s((1, lane), F32)),
            in_specs=[vmem] * 4, out_specs=[vmem] * 6, name="place",
        )(y, dx, dw, dg)
        return y, dx, dw1, dw3, dw2, dg[0]

    return jax.shard_map(
        local_step, mesh=mesh,
        in_specs=(P("ty", "tx"), P("ty", "tx"), P("tx"), P("tx", "ty"), P("tx", "ty"), P("ty", "tx")),
        out_specs=(P("ty", "tx"), P("ty", "tx"), P("tx", "ty"), P("tx", "ty"), P("ty", "tx"), P("tx")),
        check_vma=False)
```

```python
import jax
import jax.numpy as jnp
from jax import lax
from jax.experimental import pallas as pl
from jax.experimental.pallas import tpu as pltpu
from jax.sharding import PartitionSpec as P

LN_EPS = 1e-6
F32 = jnp.float32
BF16 = jnp.bfloat16
MESH = pl.DeviceIdType.MESH
LANE = 128
WIDE = LANE + LANE
ORDER = (2, 4, 3, 5, 6, 7, 1)
N_T = 8
N_Z = 4
PIECES = 8
CHUNK = 3 * LANE
ROWS = LANE // 2
PIECE_ORDER = tuple(range(4, PIECES)) + tuple(range(4))


def cols(k, width=LANE):
    return pl.ds(pl.multiple_of(k * width, width), width)


def dot(a, b):
    return jnp.dot(a, b, preferred_element_type=F32)


def dot_cols(a, b):
    return lax.dot_general(a, b, (((1,), (1,)), ((), ())), preferred_element_type=F32)


def step_kernel(x_in, dy_in, g_in, w1_in, w3_in, w2_in,
                y_out, dx_out, dw_out, dg_out,
                x_all, h_all, dy_all, gain_all, w13, w2, act, act_t, duv_t, dw, uv_all,
                m_away, m0, m1, m2, e0, e1, e2, outs, ins,
                x_rows, x_own, dg_rows, dg_plane, dg_line,
                w_send, w_recv, g_recv, in_send, in_recv, wz_send, wz_end, wz_mid, sum_send, sum_recv,
                fin_sem, red_send, red_recv, local_sem):
    z = lax.axis_index("ty")
    t = lax.axis_index("tx")
    core = lax.rem(t, 2)
    xbit = lax.rem(lax.div(t, 2), 2)
    ybit = lax.div(t, 4)
    flips = [size - 2 * size * bit for size, bit in ((1, core), (2, xbit), (4, ybit))]
    duv = x_all
    e_away = uv_all.at[pl.ds(4, 4)]

    def peer(s):
        out = t
        for bit in range(3):
            if s >> bit & 1:
                out = out + flips[bit]
        return out

    px, py, pd, pc = peer(2), peer(4), peer(6), peer(1)
    tokens = x_all.shape[0]
    half = tokens // 2
    rows = tokens // N_T

    low = lax.div(3 - z, 2)
    is_end = jnp.logical_or(z == 0, z == 3)
    is_mid = jnp.logical_or(z == 1, z == 2)
    c_end = 3 - 3 * low
    c_mid = 2 - low
    c_mid2 = 3 - c_mid
    c_end2 = 3 - c_end
    inner = z + 2 * low - 1
    outer = z - 2 * low + 1

    def rcopy(src, dst, ssem, rsem, device):
        return pltpu.make_async_remote_copy(src_ref=src, dst_ref=dst, send_sem=ssem, recv_sem=rsem,
                                            device_id=device, device_id_type=MESH)

    def wait_sent(ref, sem):
        rcopy(ref, ref, sem, sem, (z, pc)).wait_send()

    def wait_in(ref, sem):
        rcopy(ref, ref, sem, sem, (z, pc)).wait_recv()

    loc = [
        pltpu.make_async_copy(w1_in.at[:, cols(t)], w13.at[cols(t), cols(2 * z)], local_sem.at[0]),
        pltpu.make_async_copy(w3_in.at[:, cols(t)], w13.at[cols(t), cols(2 * z + 1)], local_sem.at[1]),
        pltpu.make_async_copy(w2_in.at[cols(t), :], w2.at[cols(z), cols(t)], local_sem.at[2]),
        pltpu.make_async_copy(g_in, gain_all.at[:, cols(t)], local_sem.at[3]),
        pltpu.make_async_copy(x_in, x_all.at[:, cols(t)], local_sem.at[4]),
        pltpu.make_async_copy(dy_in, dy_all.at[:, cols(t)], local_sem.at[5]),
        pltpu.make_async_copy(x_in, x_own, local_sem.at[8]),
    ]
    for c in loc:
        c.start()
    barrier = pltpu.get_barrier_semaphore()
    for s in ORDER:
        pl.semaphore_signal(barrier, inc=1, device_id=(z, peer(s)), device_id_type=MESH)
    for s in range(1, N_Z):
        pl.semaphore_signal(barrier, inc=1, device_id=(lax.rem(z + s, N_Z), t), device_id_type=MESH)
    pl.semaphore_wait(barrier, N_T - 1 + N_Z - 1)

    for s in ORDER:
        p = peer(s)
        rcopy(w1_in.at[:, cols(p)], w13.at[cols(t), cols(2 * z)], w_send.at[0], w_recv.at[s, 0], (z, p)).start()
        rcopy(w3_in.at[:, cols(p)], w13.at[cols(t), cols(2 * z + 1)], w_send.at[1], w_recv.at[s, 0], (z, p)).start()
        rcopy(w2_in.at[cols(p), :], w2.at[cols(z), cols(t)], w_send.at[2], w_recv.at[s, 1], (z, p)).start()
        rcopy(g_in, gain_all.at[:, cols(t)], w_send.at[3], g_recv.at[0], (z, p)).start()

    lo, hi = pl.ds(0, half), pl.ds(half, half)

    def move(n, src, dst, i, device):
        rcopy(src, dst, in_send.at[n], in_recv.at[n, i], (z, device)).start()

    def plane_first(n, src, full):
        move(n, src.at[lo], full.at[lo, cols(t)], 0, px)
        move(n, src.at[hi], full.at[hi, cols(t)], 2, py)
        move(n, src.at[hi], full.at[hi, cols(t)], 1, px)
        move(n, src.at[lo], full.at[lo, cols(t)], 3, py)
        move(n, src, full.at[:, cols(t)], 6, pc)

    def plane_forward(n, full):
        a, b = full.at[lo, cols(px)], full.at[hi, cols(py)]
        wait_in(a, in_recv.at[n, 0])
        move(n, a, a, 4, py)
        move(n, a, a, 7, pc)
        wait_in(b, in_recv.at[n, 2])
        move(n, b, b, 5, px)
        move(n, b, b, 7, pc)

    def plane_rest(n, full, first, many=2):
        for rr, p, i in ((hi, px, 1), (lo, py, 3), (lo, pd, 4), (hi, pd, 5))[first:first + many]:
            ref = full.at[rr, cols(p)]
            wait_in(ref, in_recv.at[n, i])
            move(n, ref, ref, 7 if i < 4 else 8, pc)

    def plane_last(n, full, group):
        wait_in(full.at[:, pl.ds(0, WIDE if group == 7 else LANE)], in_recv.at[n, group])

    plane_first(0, x_in, x_all)

    def wz_one(n, k, p, sl, device, many):
        ref = w2.at[cols(k), cols(p, many * LANE)] if n else w13.at[cols(p, many * LANE), cols(k, WIDE)]
        pair = p if many == 2 else lax.div(p, 2)
        sem = wz_end.at[sl, n] if sl < 3 else wz_mid.at[sl - 3, pair, n]
        return rcopy(ref, ref, wz_send.at[sl, n], sem, (device, t))

    def wz(k, p, sl, device):
        return tuple(wz_one(n, k, p, sl, device, 1) for n in range(2))

    def wz_own(p):
        @pl.when(is_end)
        def _():
            for c in wz(c_end, p, 3, inner):
                c.start()

        @pl.when(is_mid)
        def _():
            for c in wz(c_mid, p, 0, outer) + wz(c_mid, p, 4, inner):
                c.start()

    for c in loc[:3]:
        c.wait()
    wz_own(t)
    for s in ORDER[-1:] + ORDER[:-1]:
        p = peer(s)
        wait_in(w13.at[cols(p), cols(z, WIDE)], w_recv.at[s, 0])
        wait_in(w2.at[cols(z), cols(p)], w_recv.at[s, 1])
        wz_own(p)

    plane_forward(0, x_all)
    plane_first(1, dy_in, dy_all)

    def each_block(fn):
        lax.fori_loop(0, N_T // 2, lambda p, c: (fn(p), c)[1], 0)

    def pass_weights(n, k, from_sl, to_sl, device):
        def one(p):
            wz_one(n, k, p, from_sl, inner, 2).wait_recv()
            wz_one(n, k, p, to_sl, device, 2).start()
        each_block(one)

    def hop_one():
        pass_weights(0, c_mid2, 4, 1, outer)
        pass_weights(0, c_end, 3, 5, inner)
        pass_weights(1, c_mid2, 4, 1, outer)
        pass_weights(1, c_end, 3, 5, inner)

    def hop_two():
        pass_weights(0, c_end2, 5, 2, outer)

    def hop_three():
        pass_weights(1, c_end2, 5, 2, outer)

    @pl.when(is_mid)
    def _():
        hop_one()

    plane_rest(0, x_all, 0, 4)
    for c in loc[3:5]:
        c.wait()
    wait_in(gain_all.at[:, pl.ds(0, 7 * LANE)], g_recv.at[0])
    for group in range(6, 9):
        plane_last(0, x_all, group)

    def norm(xf):
        d = xf.shape[1]
        mu = jnp.sum(xf, axis=1, keepdims=True) / d
        sq = jnp.sum(xf * xf, axis=1, keepdims=True) / d
        r = lax.rsqrt(sq - mu * mu + LN_EPS)
        return (xf - mu) * r, r

    def norm_tile(i, carry):
        rr = pl.ds(pl.multiple_of(i * rows, rows), rows)
        xhat, _ = norm(x_all[rr, :].astype(F32))
        h_all[rr, :] = (gain_all[0:1, :] * xhat).astype(BF16)
        return carry

    def block(p):
        return pl.ds(pl.multiple_of(p * rows, rows), rows)

    def piece(p):
        if p < 4:
            return pl.ds(p * ROWS, ROWS), slice(None)
        return pl.ds(WIDE, LANE), cols(lax.div(peer(2 * p - N_T), 2), WIDE)

    def part(ref, i, p):
        return ref.at[(i, *piece(p))]

    def sum_copy(src, dst, sl, p, device):
        return rcopy(src, dst, sum_send.at[sl], sum_recv.at[sl, p], (device, t))

    def from_end(q, k, p):
        return sum_copy(part(dw, k, p), part(outs, q, p), q, p, inner)

    def end_send(q, k, pieces):
        @pl.when(is_end)
        def _():
            for p in pieces:
                from_end(q, k, p).start()

    def uv_tile(i, j):
        return 2 * i + lax.div(j, 4), cols(lax.rem(j, 4), WIDE)

    def forward_chunk(i, k, sl):
        if sl is not None:
            @pl.when(is_end)
            def _():
                wait_in(w13.at[:, cols(k, WIDE)], wz_end.at[sl, 0])

        def tile(j, c):
            rr = block(j)
            uv = dot(h_all[rr, :], w13[:, cols(k, WIDE)])
            at, cc = uv_tile(i, j)
            uv_all[at, :, cc] = uv
            u, v = uv[:, :LANE], uv[:, LANE:]
            act[rr, cols(k)] = (u * jax.nn.sigmoid(u) * v).astype(BF16)
            return c

        lax.fori_loop(0, N_T, tile, 0)

    def turn_act(k):
        def tile(j, c):
            act_t[:, block(j)] = act[block(j), cols(k)].T
            return c
        lax.fori_loop(0, N_T, tile, 0)

    n_cols = dy_all.shape[1] // (WIDE)

    def grad_down(k):
        def grad(n, c):
            grad_down_at(k, n)
            return c
        lax.fori_loop(0, n_cols, grad, 0)

    def grad_down_at(k, n):
        nn = cols(n, WIDE)
        dw[k, WIDE:, nn] = dot(act_t[...], dy_all[:, nn])

    def first_down(p):
        grad_down_at(c_mid2, lax.div(peer(2 * p - N_T), 2))
        end_send(0, c_mid2, (p,))

    def backward_chunk(i, k):
        def tile(j, c):
            rr = block(j)
            da = dot_cols(dy_all[rr, :], w2[cols(k), :])
            at, cc = uv_tile(i, j)
            uv = uv_all[at, :, cc]
            u, v = uv[:, :LANE], uv[:, LANE:]
            sig = jax.nn.sigmoid(u)
            du = (da * v * sig * (1.0 + u * (1.0 - sig))).astype(BF16)
            dv = (da * (u * sig)).astype(BF16)
            duv[rr, cols(2 * k)] = du
            duv[rr, cols(2 * k + 1)] = dv
            duv_t[0:LANE, rr] = du.T
            duv_t[LANE:, rr] = dv.T
            return c

        lax.fori_loop(0, N_T, tile, 0)

        def grad(n, c):
            nn = cols(n, WIDE)
            dw[k, 0:WIDE, nn] = dot(duv_t[...], h_all[:, nn])
            return c

        lax.fori_loop(0, n_cols, grad, 0)

    lax.fori_loop(0, N_T, norm_tile, 0)
    x_rows[...] = x_all[block(t), :]

    @pl.when(is_mid)
    def _():
        hop_two()

    forward_chunk(0, c_mid2, 1)
    plane_forward(1, dy_all)
    turn_act(c_mid2)
    loc[5].wait()
    plane_last(1, dy_all, 6)
    first_down(4)
    forward_chunk(1, c_mid, 0)

    @pl.when(is_mid)
    def _():
        hop_three()

    plane_rest(1, dy_all, 0)
    forward_chunk(2, c_end, None)
    plane_last(1, dy_all, 7)
    first_down(5)
    first_down(6)
    plane_rest(1, dy_all, 2)
    plane_last(1, dy_all, 8)
    wait_sent(x_all.at[:, pl.ds(0, 7 * LANE)], in_send.at[0])
    first_down(7)

    @pl.when(is_end)
    def _():
        wait_in(w2.at[cols(c_mid2), :], wz_end.at[1, 1])

    backward_chunk(0, c_mid2)
    end_send(0, c_mid2, PIECE_ORDER[4:])
    forward_chunk(3, c_end2, 2)

    @pl.when(is_end)
    def _():
        wait_in(w2.at[cols(c_mid), :], wz_end.at[0, 1])
        wait_in(w2.at[cols(c_end2), :], wz_end.at[2, 1])

    def stage0(away, r0, make, base):
        def body(j, c):
            fx, fy = 1 - lax.div(j, 2), 1 - lax.rem(j, 2)
            i = fx + 2 * fy
            make(away, i, pc + fx * flips[1] + fy * flips[2], False)
            rcopy(away.at[i], r0.at[i], red_send.at[base // 10], red_recv.at[base + i], (z, pc)).start()
            return c
        lax.fori_loop(0, N_T // 2, body, 0)

    def rsend(src, dst, group, sl, device):
        rcopy(src, dst, red_send.at[group], red_recv.at[sl], device).start()

    def rarrived(dst, sl):
        wait_in(dst, red_recv.at[sl])

    def stage1(r0, r1, make, base, between):
        a_half, b_half = halves(r0)
        for i in (3, 1, 2, 0):
            rarrived(r0.at[i], base + i)
            make(r0, i, (t, px, py, pd)[i], True)
            if i == 3:
                rsend(r0.at[3, a_half], r1.at[0], base // 10, base + 4, (z, px))
                rsend(r0.at[3, b_half], r1.at[1], base // 10, base + 5, (z, py))
            if i == 1:
                rsend(r0.at[1, a_half], r1.at[2], base // 10, base + 6, (z, px))
            if i == 2:
                rsend(r0.at[2, b_half], r1.at[3], base // 10, base + 7, (z, py))
            for p in between.get(i, ()):
                pass_in(0, c_mid2, p)

    def halves(r0):
        n = r0.shape[1] // 2
        return pl.ds(0, n), pl.ds(n, n)

    def stage2(r0, r1, r2, base):
        a_half, b_half = halves(r0)
        rarrived(r1.at[0], base + 4)
        r0[2, a_half] += r1[0]
        rsend(r0.at[2, a_half], r2.at[0], base // 10, base + 8, (z, py))
        rarrived(r1.at[1], base + 5)
        r0[1, b_half] += r1[1]
        rsend(r0.at[1, b_half], r2.at[1], base // 10, base + 9, (z, px))

    def stage3(r0, r1, base):
        for n, part in enumerate(halves(r0)):
            rarrived(r1.at[2 + n], base + 6 + n)
            r0[0, part] += r1[2 + n]

    def stage4(r0, r2, base):
        for n, part in enumerate(halves(r0)):
            rarrived(r2.at[n], base + 8 + n)
            r0[0, part] += r2[n]

    def make_m(ref, i, p, add):
        def tile(j, c):
            rr = cols(j, half)
            out = dot(act[rr, :], w2[:, cols(p)])
            ref[i, rr, :] = ref[i, rr, :] + out if add else out
            return c
        lax.fori_loop(0, 2, tile, 0)

    def make_dh(ref, i, p, add):
        out = dot_cols(duv[block(p), :], w13[...])
        ref[i] = ref[i] + out if add else out

    def finish(ref, i, p):
        rr, _ = piece(p)
        base = 2 * p - N_T
        for s in ORDER:
            if p < 4 or s - s % 2 == base:
                rcopy(ref.at[i, rr, cols(peer(s))], dw_out.at[t, rr], fin_sem.at[0], fin_sem.at[1], (z, peer(s))).start()
        if base <= 0:
            pltpu.make_async_copy(ref.at[i, rr, cols(t)], dw_out.at[t, rr], fin_sem.at[2]).start()

    def pass_in(q, k, p):
        @pl.when(is_mid)
        def _():
            ref = part(outs, q, p)
            sum_copy(ref, ref, q, p, outer).wait_recv()
            outs[(q, *piece(p))] += dw[(k, *piece(p))]
            sum_copy(ref, part(ins, q, p), 3 + q, p, inner).start()

    def pass_out(p):
        @pl.when(is_mid)
        def _():
            ref = part(ins, 1, p)
            sum_copy(ref, ref, 4, p, inner).wait_recv()
            ins[(1, *piece(p))] += dw[(c_end, *piece(p))]
            sum_copy(ref, ref, 5, p, outer).start()

    def last_mid(p):
        @pl.when(is_mid)
        def _():
            a, b = part(outs, 2, p), part(ins, 0, p)
            sum_copy(b, b, 3, p, inner).wait_recv()
            sum_copy(a, a, 2, p, outer).wait_recv()
            outs[(2, *piece(p))] += ins[(0, *piece(p))] + dw[(c_mid, *piece(p))]
            finish(outs, 2, p)

    def last_end(p):
        @pl.when(is_end)
        def _():
            a = part(ins, 1, p)
            sum_copy(a, a, 5, p, inner).wait_recv()
            ins[(1, *piece(p))] += dw[(c_end, *piece(p))]
            finish(ins, 1, p)

    stage0(m_away, m0, make_m, 0)
    stage1(m0, m1, make_m, 0, {3: PIECE_ORDER[:1], 2: PIECE_ORDER[1:4]})
    turn_act(c_end2)
    grad_down(c_end2)
    pass_in(0, c_mid2, 0)
    backward_chunk(3, c_end2)
    end_send(1, c_end2, PIECE_ORDER)
    turn_act(c_mid)
    grad_down(c_mid)
    pass_in(0, c_mid2, 1)
    backward_chunk(1, c_mid)
    end_send(2, c_mid, PIECE_ORDER)
    pass_in(0, c_mid2, 2)
    pass_in(0, c_mid2, 3)
    stage2(m0, m1, m2, 0)
    turn_act(c_end)
    grad_down(c_end)
    backward_chunk(2, c_end)
    for p in PIECE_ORDER[:3]:
        pass_in(1, c_end2, p)
    stage0(e_away, e0, make_dh, 10)
    pass_in(1, c_end2, PIECE_ORDER[3])
    stage1(e0, e1, make_dh, 10, {})

    def put(src, dst, local):
        c = pltpu.make_async_copy(src, dst, local_sem.at[local])
        c.start()
        loc.append(c)

    def spread(src, dst, group, local):
        for s in ORDER:
            q = peer(s)
            rsend(src.at[:, cols(q)], dst.at[block(t), :], group, group + 18, (z, q))
        put(src.at[:, cols(t)], dst.at[block(t), :], local)

    def make_y():
        stage4(m0, m2, 0)
        loc[6].wait()
        x_own[...] = (x_own[...].astype(F32) + m0[0]).astype(BF16)
        put(x_own, y_out, 6)

    def make_dx():
        stage4(e0, e2, 10)
        xhat, r = norm(x_rows[...].astype(F32))
        d = xhat.shape[1]
        dh = e0[0]
        e = dh * gain_all[0:1, :]
        e_mean = jnp.sum(e, axis=1, keepdims=True) / d
        ex_mean = jnp.sum(e * xhat, axis=1, keepdims=True) / d
        dy_rows = dy_all[block(t), :].astype(F32)
        x_rows[...] = (dy_rows + r * (e - e_mean - xhat * ex_mean)).astype(BF16)
        dg_rows[...] = jnp.sum((dh * xhat).reshape(rows // 8, 8, d), axis=0)
        for s in ORDER:
            rsend(dg_rows.at[:, cols(peer(s))], dg_plane.at[s - 1], 4, 22, (z, peer(s)))
        spread(x_rows, dx_out, 3, 7)

    def gain_plane():
        total = dg_rows[:, cols(t)]
        rarrived(dg_plane, 22)
        for s in range(1, 8):
            total = total + dg_plane[s - 1]
        dg_line[0] = total
        for s in range(1, 4):
            rsend(dg_line.at[0], dg_line.at[s], 5, 23, (lax.rem(z + s, 4), t))

    def gain_line():
        rarrived(dg_line.at[pl.ds(1, 3)], 23)
        parts = [dg_line[lax.rem(z - s + 4, 4)] for s in range(4)]
        dg_out[...] = sum(parts[1:], parts[0])

    plan = [(84, lambda: stage3(m0, m1, 0)), (96, make_y),
            (109, lambda: stage2(e0, e1, e2, 10)), (120, lambda: stage3(e0, e1, 10)),
            (131, make_dx), (147, gain_plane), (157, gain_line)]
    done = 78.4
    for p in PIECE_ORDER:
        done += 5.6 if p < 4 else 2.8
        if p < 4:
            plan.append((done, lambda p=p: pass_in(1, c_end2, p)))
        late = max(done, 89.6)
        plan.append((late + 6.6, lambda p=p: pass_out(p)))
        plan.append((late + 13, lambda p=p: last_end(p)))
        plan.append((done + 33.7, lambda p=p: last_mid(p)))
    for _, fn in sorted(plan, key=lambda e: e[0]):
        fn()

    seven = pl.ds(0, 7 * LANE)
    rarrived(dx_out.at[pl.ds(0, 7 * rows), :], 21)
    wait_in(dw_out.at[pl.ds(0, 7)], fin_sem.at[1])
    pltpu.make_async_copy(dw_out.at[0], dw_out.at[0], fin_sem.at[2]).wait()
    for c in loc[7:]:
        c.wait()
    wait_sent(dw_out.at[pl.ds(0, 7)], fin_sem.at[0])
    for n in range(3):
        wait_sent(w13.at[pl.ds(0, LANE), seven], w_send.at[n])
    wait_sent(gain_all.at[:, seven], w_send.at[3])
    wait_sent(dy_all.at[:, seven], in_send.at[1])
    most = uv_all.at[pl.ds(0, 7)]
    for n, ref in enumerate((most, most, None, x_rows.at[:, seven],
                             dg_rows.at[:, seven], dg_line.at[pl.ds(1, 3)])):
        if ref is not None:
            wait_sent(ref, red_send.at[n])

    def chunk_sent(sl):
        wait_sent(w13.at[:, cols(0, WIDE)], wz_send.at[sl, 0])
        wait_sent(w2.at[cols(0), :], wz_send.at[sl, 1])

    @pl.when(is_end)
    def _():
        chunk_sent(3)
        for q in range(3):
            wait_sent(dw.at[0], sum_send.at[q])

    @pl.when(is_mid)
    def _():
        for sl in range(6):
            if sl != 3:
                chunk_sent(sl)
        for q in range(3, 6):
            wait_sent(dw.at[0], sum_send.at[q])


def place_kernel(y_in, dx_in, dw_in, dg_in, y_out, dx_out, dw1_out, dw3_out, dw2_out, dg_out):
    y_out[...] = y_in[...]
    dx_out[...] = dx_in[...]
    for s in range(N_T):
        at = slice(s * LANE, (s + 1) * LANE)
        dw1_out[:, at] = dw_in[s, 0:LANE].T
        dw3_out[:, at] = dw_in[s, LANE:WIDE].T
        dw2_out[at, :] = dw_in[s, WIDE:]
    dg_out[...] = jnp.sum(dg_in[...], axis=0, keepdims=True)


def solution(mesh):
    def local_step(x_blk, dy_blk, gain_blk, w1_blk, w3_blk, w2_blk):
        tokens, lane = x_blk.shape
        d = lane * N_T
        f = w1_blk.shape[1] // N_T * N_Z
        rows = tokens // N_T
        any_spec = pl.BlockSpec(memory_space=pl.ANY)
        vmem = pl.BlockSpec(memory_space=pltpu.VMEM)
        s = jax.ShapeDtypeStruct
        V = pltpu.VMEM
        dma = pltpu.SemaphoreType.DMA
        def red(r, c):
            half = V((2, r // 2, c), F32)
            return [V((4, r, c), F32), V((4, r // 2, c), F32), half]
        y, dx, dw, dg = pl.pallas_call(
            step_kernel,
            out_shape=(s((tokens, lane), BF16), s((tokens, lane), BF16), s((N_T, CHUNK, lane), F32), s((8, lane), F32)),
            in_specs=[any_spec] * 6,
            out_specs=[any_spec] * 3 + [vmem],
            scratch_shapes=[
                V((tokens, d), BF16), V((tokens, d), BF16), V((tokens, d), BF16), V((1, d), F32),
                V((d, 2 * f), BF16), V((f, d), BF16), V((tokens, f), BF16), V((lane, tokens), BF16),
                V((WIDE, tokens), BF16), V((N_Z, CHUNK, d), F32), V((N_T, rows, d), F32), V((4, tokens, lane), F32)] + red(tokens, lane) + red(rows, d) + [
                V((3, CHUNK, d), F32), V((2, CHUNK, d), F32),
                V((rows, d), BF16), V((tokens, lane), BF16), V((8, d), F32),
                V((7, 8, lane), F32), V((4, 8, lane), F32),
                dma((4,)), dma((N_T, 2)), dma((1,)), dma((2,)), dma((2, 9)), dma((6, 2)), dma((3, 2)),
                dma((3, N_T // 2, 2)), dma((6,)), dma((6, PIECES)), dma((3,)), dma((6,)), dma((24,)), dma((9,))],
            compiler_params=pltpu.CompilerParams(collective_id=0, has_side_effects=True, vmem_limit_bytes=67043328),
            name="step",
        )(x_blk, dy_blk, gain_blk[None, :], w1_blk, w3_blk, w2_blk)
        f_z = w1_blk.shape[1]
        y, dx, dw1, dw3, dw2, dg = pl.pallas_call(
            place_kernel,
            out_shape=(s((tokens, lane), BF16), s((tokens, lane), BF16), s((lane, f_z), F32), s((lane, f_z), F32),
                       s((f_z, lane), F32), s((1, lane), F32)),
            in_specs=[vmem] * 4, out_specs=[vmem] * 6, name="place",
        )(y, dx, dw, dg)
        return y, dx, dw1, dw3, dw2, dg[0]

    return jax.shard_map(
        local_step, mesh=mesh,
        in_specs=(P("ty", "tx"), P("ty", "tx"), P("tx"), P("tx", "ty"), P("tx", "ty"), P("ty", "tx")),
        out_specs=(P("ty", "tx"), P("ty", "tx"), P("tx", "ty"), P("tx", "ty"), P("ty", "tx"), P("tx")),
        check_vma=False)
```

```python
import jax
import jax.numpy as jnp
from jax import lax
from jax.experimental import pallas as pl
from jax.experimental.pallas import tpu as pltpu
from jax.sharding import PartitionSpec as P

LN_EPS = 1e-6
F32 = jnp.float32
BF16 = jnp.bfloat16
MESH = pl.DeviceIdType.MESH
LANE = 128
WIDE = LANE + LANE
ORDER = (2, 4, 3, 5, 6, 7, 1)
N_T = 8
N_Z = 4
PIECES = 8
CHUNK = 3 * LANE
ROWS = LANE // 2
PIECE_ORDER = tuple(range(4, PIECES)) + tuple(range(4))


def cols(k, width=LANE):
    return pl.ds(pl.multiple_of(k * width, width), width)


def dot(a, b):
    return jnp.dot(a, b, preferred_element_type=F32)


def dot_cols(a, b):
    return lax.dot_general(a, b, (((1,), (1,)), ((), ())), preferred_element_type=F32)


def step_kernel(x_in, dy_in, g_in, w1_in, w3_in, w2_in,
                y_out, dx_out, dw_out, dg_out,
                x_all, h_all, dy_all, gain_all, w13, w2, act, act_t, duv_t, dw, uv_all,
                m_away, m0, m1, m2, e0, e1, e2, outs, ins,
                x_rows, x_own, dg_rows, dg_plane, dg_line,
                w_send, w_recv, g_recv, in_send, in_recv, wz_send, wz_end, wz_mid, sum_send, sum_recv,
                fin_sem, red_send, red_recv, local_sem):
    z = lax.axis_index("ty")
    t = lax.axis_index("tx")
    core = lax.rem(t, 2)
    xbit = lax.rem(lax.div(t, 2), 2)
    ybit = lax.div(t, 4)
    flips = [size - 2 * size * bit for size, bit in ((1, core), (2, xbit), (4, ybit))]
    duv = x_all
    e_away = uv_all.at[pl.ds(4, 4)]

    def peer(s):
        out = t
        for bit in range(3):
            if s >> bit & 1:
                out = out + flips[bit]
        return out

    px, py, pd, pc = peer(2), peer(4), peer(6), peer(1)
    tokens = x_all.shape[0]
    half = tokens // 2
    rows = tokens // N_T

    low = lax.div(3 - z, 2)
    is_end = jnp.logical_or(z == 0, z == 3)
    is_mid = jnp.logical_or(z == 1, z == 2)
    c_end = 3 - 3 * low
    c_mid = 2 - low
    c_mid2 = 3 - c_mid
    c_end2 = 3 - c_end
    inner = z + 2 * low - 1
    outer = z - 2 * low + 1

    def rcopy(src, dst, ssem, rsem, device):
        return pltpu.make_async_remote_copy(src_ref=src, dst_ref=dst, send_sem=ssem, recv_sem=rsem,
                                            device_id=device, device_id_type=MESH)

    def wait_sent(ref, sem):
        rcopy(ref, ref, sem, sem, (z, pc)).wait_send()

    def wait_in(ref, sem):
        rcopy(ref, ref, sem, sem, (z, pc)).wait_recv()

    loc = [
        pltpu.make_async_copy(w1_in.at[:, cols(t)], w13.at[cols(t), cols(2 * z)], local_sem.at[0]),
        pltpu.make_async_copy(w3_in.at[:, cols(t)], w13.at[cols(t), cols(2 * z + 1)], local_sem.at[1]),
        pltpu.make_async_copy(w2_in.at[cols(t), :], w2.at[cols(z), cols(t)], local_sem.at[2]),
        pltpu.make_async_copy(g_in, gain_all.at[:, cols(t)], local_sem.at[3]),
        pltpu.make_async_copy(x_in, x_all.at[:, cols(t)], local_sem.at[4]),
        pltpu.make_async_copy(dy_in, dy_all.at[:, cols(t)], local_sem.at[5]),
        pltpu.make_async_copy(x_in, x_own, local_sem.at[8]),
    ]
    for c in loc:
        c.start()
    barrier = pltpu.get_barrier_semaphore()
    for s in ORDER:
        pl.semaphore_signal(barrier, inc=1, device_id=(z, peer(s)), device_id_type=MESH)
    for s in range(1, N_Z):
        pl.semaphore_signal(barrier, inc=1, device_id=(lax.rem(z + s, N_Z), t), device_id_type=MESH)
    pl.semaphore_wait(barrier, N_T - 1 + N_Z - 1)

    for s in ORDER:
        p = peer(s)
        rcopy(w1_in.at[:, cols(p)], w13.at[cols(t), cols(2 * z)], w_send.at[0], w_recv.at[s, 0], (z, p)).start()
        rcopy(w3_in.at[:, cols(p)], w13.at[cols(t), cols(2 * z + 1)], w_send.at[1], w_recv.at[s, 0], (z, p)).start()
        rcopy(w2_in.at[cols(p), :], w2.at[cols(z), cols(t)], w_send.at[2], w_recv.at[s, 1], (z, p)).start()
        rcopy(g_in, gain_all.at[:, cols(t)], w_send.at[3], g_recv.at[0], (z, p)).start()

    lo, hi = pl.ds(0, half), pl.ds(half, half)

    def move(n, src, dst, i, device):
        rcopy(src, dst, in_send.at[n], in_recv.at[n, i], (z, device)).start()

    def plane_first(n, src, full):
        move(n, src.at[lo], full.at[lo, cols(t)], 0, px)
        move(n, src.at[hi], full.at[hi, cols(t)], 2, py)
        move(n, src.at[hi], full.at[hi, cols(t)], 1, px)
        move(n, src.at[lo], full.at[lo, cols(t)], 3, py)
        move(n, src, full.at[:, cols(t)], 6, pc)

    def plane_forward(n, full):
        a, b = full.at[lo, cols(px)], full.at[hi, cols(py)]
        wait_in(a, in_recv.at[n, 0])
        move(n, a, a, 4, py)
        move(n, a, a, 7, pc)
        wait_in(b, in_recv.at[n, 2])
        move(n, b, b, 5, px)
        move(n, b, b, 7, pc)

    def plane_rest(n, full, first, many=2):
        for rr, p, i in ((hi, px, 1), (lo, py, 3), (lo, pd, 4), (hi, pd, 5))[first:first + many]:
            ref = full.at[rr, cols(p)]
            wait_in(ref, in_recv.at[n, i])
            move(n, ref, ref, 7 if i < 4 else 8, pc)

    def plane_last(n, full, group):
        wait_in(full.at[:, pl.ds(0, WIDE if group == 7 else LANE)], in_recv.at[n, group])

    plane_first(0, x_in, x_all)

    def wz_one(n, k, p, sl, device, many):
        ref = w2.at[cols(k), cols(p, many * LANE)] if n else w13.at[cols(p, many * LANE), cols(k, WIDE)]
        pair = p if many == 2 else lax.div(p, 2)
        sem = wz_end.at[sl, n] if sl < 3 else wz_mid.at[sl - 3, pair, n]
        return rcopy(ref, ref, wz_send.at[sl, n], sem, (device, t))

    def wz(k, p, sl, device):
        return tuple(wz_one(n, k, p, sl, device, 1) for n in range(2))

    def wz_own(p):
        @pl.when(is_end)
        def _():
            for c in wz(c_end, p, 3, inner):
                c.start()

        @pl.when(is_mid)
        def _():
            for c in wz(c_mid, p, 0, outer) + wz(c_mid, p, 4, inner):
                c.start()

    for c in loc[:3]:
        c.wait()
    wz_own(t)
    for s in ORDER[-1:] + ORDER[:-1]:
        p = peer(s)
        wait_in(w13.at[cols(p), cols(z, WIDE)], w_recv.at[s, 0])
        wait_in(w2.at[cols(z), cols(p)], w_recv.at[s, 1])
        wz_own(p)

    plane_forward(0, x_all)
    plane_first(1, dy_in, dy_all)

    def each_block(fn):
        lax.fori_loop(0, N_T // 2, lambda p, c: (fn(p), c)[1], 0)

    def pass_weights(n, k, from_sl, to_sl, device):
        def one(p):
            wz_one(n, k, p, from_sl, inner, 2).wait_recv()
            wz_one(n, k, p, to_sl, device, 2).start()
        each_block(one)

    def hop_one():
        pass_weights(0, c_mid2, 4, 1, outer)
        pass_weights(0, c_end, 3, 5, inner)
        pass_weights(1, c_mid2, 4, 1, outer)
        pass_weights(1, c_end, 3, 5, inner)

    def hop_two():
        pass_weights(0, c_end2, 5, 2, outer)

    def hop_three():
        pass_weights(1, c_end2, 5, 2, outer)

    @pl.when(is_mid)
    def _():
        hop_one()

    plane_rest(0, x_all, 0, 4)
    for c in loc[3:5]:
        c.wait()
    wait_in(gain_all.at[:, pl.ds(0, 7 * LANE)], g_recv.at[0])
    for group in range(6, 9):
        plane_last(0, x_all, group)

    def norm(xf):
        d = xf.shape[1]
        mu = jnp.sum(xf, axis=1, keepdims=True) / d
        sq = jnp.sum(xf * xf, axis=1, keepdims=True) / d
        r = lax.rsqrt(sq - mu * mu + LN_EPS)
        return (xf - mu) * r, r

    def norm_tile(i, carry):
        rr = pl.ds(pl.multiple_of(i * rows, rows), rows)
        xhat, _ = norm(x_all[rr, :].astype(F32))
        h_all[rr, :] = (gain_all[0:1, :] * xhat).astype(BF16)
        return carry

    def block(p):
        return pl.ds(pl.multiple_of(p * rows, rows), rows)

    def piece(p):
        if p < 4:
            return pl.ds(p * ROWS, ROWS), slice(None)
        return pl.ds(WIDE, LANE), cols(lax.div(peer(2 * p - N_T), 2), WIDE)

    def part(ref, i, p):
        return ref.at[(i, *piece(p))]

    def sum_copy(src, dst, sl, p, device):
        return rcopy(src, dst, sum_send.at[sl], sum_recv.at[sl, p], (device, t))

    def from_end(q, k, p):
        return sum_copy(part(dw, k, p), part(outs, q, p), q, p, inner)

    def end_send(q, k, pieces):
        @pl.when(is_end)
        def _():
            for p in pieces:
                from_end(q, k, p).start()

    def uv_tile(i, j):
        return 2 * i + lax.div(j, 4), cols(lax.rem(j, 4), WIDE)

    def forward_chunk(i, k, sl):
        if sl is not None:
            @pl.when(is_end)
            def _():
                wait_in(w13.at[:, cols(k, WIDE)], wz_end.at[sl, 0])

        def tile(j, c):
            rr = block(j)
            uv = dot(h_all[rr, :], w13[:, cols(k, WIDE)])
            at, cc = uv_tile(i, j)
            uv_all[at, :, cc] = uv
            u, v = uv[:, :LANE], uv[:, LANE:]
            act[rr, cols(k)] = (u * jax.nn.sigmoid(u) * v).astype(BF16)
            return c

        lax.fori_loop(0, N_T, tile, 0)

    def turn_act(k):
        def tile(j, c):
            act_t[:, block(j)] = act[block(j), cols(k)].T
            return c
        lax.fori_loop(0, N_T, tile, 0)

    n_cols = dy_all.shape[1] // (WIDE)

    def grad_down(k):
        def grad(n, c):
            grad_down_at(k, n)
            return c
        lax.fori_loop(0, n_cols, grad, 0)

    def grad_down_at(k, n):
        nn = cols(n, WIDE)
        dw[k, WIDE:, nn] = dot(act_t[...], dy_all[:, nn])

    def first_down(p):
        grad_down_at(c_mid2, lax.div(peer(2 * p - N_T), 2))
        end_send(0, c_mid2, (p,))

    def backward_chunk(i, k):
        def tile(j, c):
            rr = block(j)
            da = dot_cols(dy_all[rr, :], w2[cols(k), :])
            at, cc = uv_tile(i, j)
            uv = uv_all[at, :, cc]
            u, v = uv[:, :LANE], uv[:, LANE:]
            sig = jax.nn.sigmoid(u)
            du = (da * v * sig * (1.0 + u * (1.0 - sig))).astype(BF16)
            dv = (da * (u * sig)).astype(BF16)
            duv[rr, cols(2 * k)] = du
            duv[rr, cols(2 * k + 1)] = dv
            duv_t[0:LANE, rr] = du.T
            duv_t[LANE:, rr] = dv.T
            return c

        lax.fori_loop(0, N_T, tile, 0)

        def grad(n, c):
            nn = cols(n, WIDE)
            dw[k, 0:WIDE, nn] = dot(duv_t[...], h_all[:, nn])
            return c

        lax.fori_loop(0, n_cols, grad, 0)

    lax.fori_loop(0, N_T, norm_tile, 0)
    x_rows[...] = x_all[block(t), :]

    @pl.when(is_mid)
    def _():
        hop_two()

    forward_chunk(0, c_mid2, 1)
    plane_forward(1, dy_all)
    turn_act(c_mid2)
    loc[5].wait()
    plane_last(1, dy_all, 6)
    first_down(4)
    forward_chunk(1, c_mid, 0)

    @pl.when(is_mid)
    def _():
        hop_three()

    plane_rest(1, dy_all, 0)
    forward_chunk(2, c_end, None)
    plane_last(1, dy_all, 7)
    first_down(5)
    first_down(6)
    plane_rest(1, dy_all, 2)
    plane_last(1, dy_all, 8)
    wait_sent(x_all.at[:, pl.ds(0, 7 * LANE)], in_send.at[0])
    first_down(7)

    @pl.when(is_end)
    def _():
        wait_in(w2.at[cols(c_mid2), :], wz_end.at[1, 1])

    def stage0(away, r0, make, base):
        def body(j, c):
            fx, fy = 1 - lax.div(j, 2), 1 - lax.rem(j, 2)
            i = fx + 2 * fy
            make(away, i, pc + fx * flips[1] + fy * flips[2], False)
            rcopy(away.at[i], r0.at[i], red_send.at[base // 10], red_recv.at[base + i], (z, pc)).start()
            return c
        lax.fori_loop(0, N_T // 2, body, 0)

    def rsend(src, dst, group, sl, device):
        rcopy(src, dst, red_send.at[group], red_recv.at[sl], device).start()

    def rarrived(dst, sl):
        wait_in(dst, red_recv.at[sl])

    def stage1(r0, r1, make, base, between):
        a_half, b_half = halves(r0)
        for i in (3, 1, 2, 0):
            rarrived(r0.at[i], base + i)
            make(r0, i, (t, px, py, pd)[i], True)
            if i == 3:
                rsend(r0.at[3, a_half], r1.at[0], base // 10, base + 4, (z, px))
                rsend(r0.at[3, b_half], r1.at[1], base // 10, base + 5, (z, py))
            if i == 1:
                rsend(r0.at[1, a_half], r1.at[2], base // 10, base + 6, (z, px))
            if i == 2:
                rsend(r0.at[2, b_half], r1.at[3], base // 10, base + 7, (z, py))
            for p in between.get(i, ()):
                pass_in(0, c_mid2, p)

    def halves(r0):
        n = r0.shape[1] // 2
        return pl.ds(0, n), pl.ds(n, n)

    def stage2(r0, r1, r2, base):
        a_half, b_half = halves(r0)
        rarrived(r1.at[0], base + 4)
        r0[2, a_half] += r1[0]
        rsend(r0.at[2, a_half], r2.at[0], base // 10, base + 8, (z, py))
        rarrived(r1.at[1], base + 5)
        r0[1, b_half] += r1[1]
        rsend(r0.at[1, b_half], r2.at[1], base // 10, base + 9, (z, px))

    def stage3(r0, r1, base):
        for n, part in enumerate(halves(r0)):
            rarrived(r1.at[2 + n], base + 6 + n)
            r0[0, part] += r1[2 + n]

    def stage4(r0, r2, base):
        for n, part in enumerate(halves(r0)):
            rarrived(r2.at[n], base + 8 + n)
            r0[0, part] += r2[n]

    def make_m(ref, i, p, add):
        out = dot(act[...], w2[:, cols(p)])
        ref[i] = ref[i] + out if add else out

    def make_dh(ref, i, p, add):
        out = dot_cols(duv[block(p), :], w13[...])
        ref[i] = ref[i] + out if add else out

    def finish(ref, i, p):
        rr, _ = piece(p)
        base = 2 * p - N_T
        for s in ORDER:
            if p < 4 or s - s % 2 == base:
                rcopy(ref.at[i, rr, cols(peer(s))], dw_out.at[t, rr], fin_sem.at[0], fin_sem.at[1], (z, peer(s))).start()
        if base <= 0:
            pltpu.make_async_copy(ref.at[i, rr, cols(t)], dw_out.at[t, rr], fin_sem.at[2]).start()

    def pass_in(q, k, p):
        @pl.when(is_mid)
        def _():
            ref = part(outs, q, p)
            sum_copy(ref, ref, q, p, outer).wait_recv()
            outs[(q, *piece(p))] += dw[(k, *piece(p))]
            sum_copy(ref, part(ins, q, p), 3 + q, p, inner).start()

    def pass_out(p):
        @pl.when(is_mid)
        def _():
            ref = part(ins, 1, p)
            sum_copy(ref, ref, 4, p, inner).wait_recv()
            ins[(1, *piece(p))] += dw[(c_end, *piece(p))]
            sum_copy(ref, ref, 5, p, outer).start()

    def last_mid(p):
        @pl.when(is_mid)
        def _():
            a, b = part(outs, 2, p), part(ins, 0, p)
            sum_copy(b, b, 3, p, inner).wait_recv()
            sum_copy(a, a, 2, p, outer).wait_recv()
            outs[(2, *piece(p))] += ins[(0, *piece(p))] + dw[(c_mid, *piece(p))]
            finish(outs, 2, p)

    def last_end(p):
        @pl.when(is_end)
        def _():
            a = part(ins, 1, p)
            sum_copy(a, a, 5, p, inner).wait_recv()
            ins[(1, *piece(p))] += dw[(c_end, *piece(p))]
            finish(ins, 1, p)

    def start_m():
        forward_chunk(3, c_end2, 2)

        @pl.when(is_end)
        def _():
            wait_in(w2.at[cols(c_mid), :], wz_end.at[0, 1])
            wait_in(w2.at[cols(c_end2), :], wz_end.at[2, 1])

        stage0(m_away, m0, make_m, 0)
        stage1(m0, m1, make_m, 0, {3: PIECE_ORDER[:1], 2: PIECE_ORDER[1:4]})

    pl.when(is_mid)(start_m)
    backward_chunk(0, c_mid2)
    end_send(0, c_mid2, PIECE_ORDER[4:])
    pl.when(is_end)(start_m)
    turn_act(c_end2)
    grad_down(c_end2)
    pass_in(0, c_mid2, 0)
    backward_chunk(3, c_end2)
    end_send(1, c_end2, PIECE_ORDER)
    turn_act(c_mid)
    grad_down(c_mid)
    pass_in(0, c_mid2, 1)
    backward_chunk(1, c_mid)
    end_send(2, c_mid, PIECE_ORDER)
    pass_in(0, c_mid2, 2)
    pass_in(0, c_mid2, 3)
    stage2(m0, m1, m2, 0)
    turn_act(c_end)
    grad_down(c_end)
    backward_chunk(2, c_end)
    for p in PIECE_ORDER[:3]:
        pass_in(1, c_end2, p)
    stage0(e_away, e0, make_dh, 10)
    pass_in(1, c_end2, PIECE_ORDER[3])
    stage1(e0, e1, make_dh, 10, {})

    def put(src, dst, local):
        c = pltpu.make_async_copy(src, dst, local_sem.at[local])
        c.start()
        loc.append(c)

    def spread(src, dst, group, local):
        for s in ORDER:
            q = peer(s)
            rsend(src.at[:, cols(q)], dst.at[block(t), :], group, group + 18, (z, q))
        put(src.at[:, cols(t)], dst.at[block(t), :], local)

    def make_y():
        stage4(m0, m2, 0)
        loc[6].wait()
        x_own[...] = (x_own[...].astype(F32) + m0[0]).astype(BF16)
        put(x_own, y_out, 6)

    def make_dx():
        stage4(e0, e2, 10)
        xhat, r = norm(x_rows[...].astype(F32))
        d = xhat.shape[1]
        dh = e0[0]
        e = dh * gain_all[0:1, :]
        e_mean = jnp.sum(e, axis=1, keepdims=True) / d
        ex_mean = jnp.sum(e * xhat, axis=1, keepdims=True) / d
        dy_rows = dy_all[block(t), :].astype(F32)
        x_rows[...] = (dy_rows + r * (e - e_mean - xhat * ex_mean)).astype(BF16)
        dg_rows[...] = jnp.sum((dh * xhat).reshape(rows // 8, 8, d), axis=0)
        for s in ORDER:
            rsend(dg_rows.at[:, cols(peer(s))], dg_plane.at[s - 1], 4, 22, (z, peer(s)))
        spread(x_rows, dx_out, 3, 7)

    def gain_plane():
        total = dg_rows[:, cols(t)]
        rarrived(dg_plane, 22)
        for s in range(1, 8):
            total = total + dg_plane[s - 1]
        dg_line[0] = total
        for s in range(1, 4):
            rsend(dg_line.at[0], dg_line.at[s], 5, 23, (lax.rem(z + s, 4), t))

    def gain_line():
        rarrived(dg_line.at[pl.ds(1, 3)], 23)
        parts = [dg_line[lax.rem(z - s + 4, 4)] for s in range(4)]
        dg_out[...] = sum(parts[1:], parts[0])

    plan = [(84, lambda: stage3(m0, m1, 0)), (96, make_y),
            (101.9, lambda: stage2(e0, e1, e2, 10)), (120, lambda: stage3(e0, e1, 10)),
            (123, make_dx), (147, gain_plane), (157, gain_line)]
    done = 78.4
    for p in PIECE_ORDER:
        done += 5.6 if p < 4 else 2.8
        if p < 4:
            plan.append((done, lambda p=p: pass_in(1, c_end2, p)))
        late = max(done, 89.6)
        plan.append((late + 6.6, lambda p=p: pass_out(p)))
        plan.append((late + 13, lambda p=p: last_end(p)))
        plan.append((done + 33.7, lambda p=p: last_mid(p)))
    for _, fn in sorted(plan, key=lambda e: e[0]):
        fn()

    seven = pl.ds(0, 7 * LANE)
    rarrived(dx_out.at[pl.ds(0, 7 * rows), :], 21)
    wait_in(dw_out.at[pl.ds(0, 7)], fin_sem.at[1])
    pltpu.make_async_copy(dw_out.at[0], dw_out.at[0], fin_sem.at[2]).wait()
    for c in loc[7:]:
        c.wait()
    wait_sent(dw_out.at[pl.ds(0, 7)], fin_sem.at[0])
    for n in range(3):
        wait_sent(w13.at[pl.ds(0, LANE), seven], w_send.at[n])
    wait_sent(gain_all.at[:, seven], w_send.at[3])
    wait_sent(dy_all.at[:, seven], in_send.at[1])
    most = uv_all.at[pl.ds(0, 7)]
    for n, ref in enumerate((most, most, None, x_rows.at[:, seven],
                             dg_rows.at[:, seven], dg_line.at[pl.ds(1, 3)])):
        if ref is not None:
            wait_sent(ref, red_send.at[n])

    def chunk_sent(sl):
        wait_sent(w13.at[:, cols(0, WIDE)], wz_send.at[sl, 0])
        wait_sent(w2.at[cols(0), :], wz_send.at[sl, 1])

    @pl.when(is_end)
    def _():
        chunk_sent(3)
        for q in range(3):
            wait_sent(dw.at[0], sum_send.at[q])

    @pl.when(is_mid)
    def _():
        for sl in range(6):
            if sl != 3:
                chunk_sent(sl)
        for q in range(3, 6):
            wait_sent(dw.at[0], sum_send.at[q])


def place_kernel(y_in, dx_in, dw_in, dg_in, y_out, dx_out, dw1_out, dw3_out, dw2_out, dg_out):
    y_out[...] = y_in[...]
    dx_out[...] = dx_in[...]
    for s in range(N_T):
        at = slice(s * LANE, (s + 1) * LANE)
        dw1_out[:, at] = dw_in[s, 0:LANE].T
        dw3_out[:, at] = dw_in[s, LANE:WIDE].T
        dw2_out[at, :] = dw_in[s, WIDE:]
    dg_out[...] = jnp.sum(dg_in[...], axis=0, keepdims=True)


def solution(mesh):
    def local_step(x_blk, dy_blk, gain_blk, w1_blk, w3_blk, w2_blk):
        tokens, lane = x_blk.shape
        d = lane * N_T
        f = w1_blk.shape[1] // N_T * N_Z
        rows = tokens // N_T
        any_spec = pl.BlockSpec(memory_space=pl.ANY)
        vmem = pl.BlockSpec(memory_space=pltpu.VMEM)
        s = jax.ShapeDtypeStruct
        V = pltpu.VMEM
        dma = pltpu.SemaphoreType.DMA
        def red(r, c):
            half = V((2, r // 2, c), F32)
            return [V((4, r, c), F32), V((4, r // 2, c), F32), half]
        y, dx, dw, dg = pl.pallas_call(
            step_kernel,
            out_shape=(s((tokens, lane), BF16), s((tokens, lane), BF16), s((N_T, CHUNK, lane), F32), s((8, lane), F32)),
            in_specs=[any_spec] * 6,
            out_specs=[any_spec] * 3 + [vmem],
            scratch_shapes=[
                V((tokens, d), BF16), V((tokens, d), BF16), V((tokens, d), BF16), V((1, d), F32),
                V((d, 2 * f), BF16), V((f, d), BF16), V((tokens, f), BF16), V((lane, tokens), BF16),
                V((WIDE, tokens), BF16), V((N_Z, CHUNK, d), F32), V((N_T, rows, d), F32), V((4, tokens, lane), F32)] + red(tokens, lane) + red(rows, d) + [
                V((3, CHUNK, d), F32), V((2, CHUNK, d), F32),
                V((rows, d), BF16), V((tokens, lane), BF16), V((8, d), F32),
                V((7, 8, lane), F32), V((4, 8, lane), F32),
                dma((4,)), dma((N_T, 2)), dma((1,)), dma((2,)), dma((2, 9)), dma((6, 2)), dma((3, 2)),
                dma((3, N_T // 2, 2)), dma((6,)), dma((6, PIECES)), dma((3,)), dma((6,)), dma((24,)), dma((9,))],
            compiler_params=pltpu.CompilerParams(collective_id=0, has_side_effects=True, vmem_limit_bytes=67043328),
            name="step",
        )(x_blk, dy_blk, gain_blk[None, :], w1_blk, w3_blk, w2_blk)
        f_z = w1_blk.shape[1]
        y, dx, dw1, dw3, dw2, dg = pl.pallas_call(
            place_kernel,
            out_shape=(s((tokens, lane), BF16), s((tokens, lane), BF16), s((lane, f_z), F32), s((lane, f_z), F32),
                       s((f_z, lane), F32), s((1, lane), F32)),
            in_specs=[vmem] * 4, out_specs=[vmem] * 6, name="place",
        )(y, dx, dw, dg)
        return y, dx, dw1, dw3, dw2, dg[0]

    return jax.shard_map(
        local_step, mesh=mesh,
        in_specs=(P("ty", "tx"), P("ty", "tx"), P("tx"), P("tx", "ty"), P("tx", "ty"), P("ty", "tx")),
        out_specs=(P("ty", "tx"), P("ty", "tx"), P("tx", "ty"), P("tx", "ty"), P("ty", "tx"), P("tx")),
        check_vma=False)
```
